32 devices in a mesh: dp: 1 (over z), cp: 32 (over y, x, core).
Axes of the slice: x: 4, y: 4, z: 1, core: 2. Of those that a mesh axis runs over, the one named last changes fastest.
The devices are a block of a 4x4x8 slice.
Arguments:
- x: bfloat16 [8, 6144], P('dp')
- w_dq: bfloat16 [6144, 1536], replicated
- g_q: float32 [1536], replicated
- w_uq: bfloat16 [1536, 12288], replicated
- w_dkv: bfloat16 [6144, 576], replicated
- g_kv: float32 [512], replicated
- w_uk: bfloat16 [512, 64, 128], replicated
- w_uv: bfloat16 [512, 64, 128], replicated
- w_o: bfloat16 [8192, 6144], replicated
- cache_c: bfloat16 [8, 65536, 512], P('dp', 'cp')
- cache_kr: bfloat16 [8, 65536, 64], P('dp', 'cp')
- ctx_len: int32 [8], P('dp')
Outputs:
- output 1: bfloat16 [8, 6144], P('dp')
- output 2: bfloat16 [8, 512], P('dp')
- output 3: bfloat16 [8, 64], P('dp')
All inputs are finite; a program needn't handle non-finite values.
Results may differ from the reference program's by a relative error of at most 0.00615798.
Values sent between devices are 32-bit elements.
A program may use at most 768 MiB of HBM per device.

```python
import jax
import jax.numpy as jnp
from jax import lax

BATCH = 8
T_DEV = 2048
GROUP_SIZE = 32
D_MODEL = 6144
HEADS = 64
Q_LORA = 1536
LATENT = 512
NOPE_DIM = 128
ROPE_DIM = 64
V_DIM = 128

SEQ = T_DEV * GROUP_SIZE
QK_DIM = NOPE_DIM + ROPE_DIM
NORM_EPS = 1e-6
ROPE_THETA = 10000.0


def rms_norm(values, gain_vec):
    mean_sq = jnp.mean(jnp.square(values), axis=-1, keepdims=True)
    return values * lax.rsqrt(mean_sq + NORM_EPS) * gain_vec


def rope_tables(positions):
    half_dim = ROPE_DIM // 2
    inv_freq = ROPE_THETA ** (-2.0 * jnp.arange(half_dim, dtype=jnp.float32) / ROPE_DIM)
    angles = positions.astype(jnp.float32)[..., None] * inv_freq
    return jnp.cos(angles), jnp.sin(angles)


def rope_rotate(values, cos_tab, sin_tab):
    half_dim = values.shape[-1] // 2
    lo_half = values[..., :half_dim]
    hi_half = values[..., half_dim:]
    return jnp.concatenate([lo_half * cos_tab - hi_half * sin_tab, hi_half * cos_tab + lo_half * sin_tab], axis=-1)


def setup_inputs(seed: int = 0, part: int = 0) -> dict:
    shared_keys = jax.random.split(jax.random.key(seed), 8)
    part_keys = jax.random.split(jax.random.fold_in(jax.random.key(seed + 1), part), 8)

    def draw_normal(key, shape, std):
        return jax.random.normal(key, shape, jnp.float32) * std

    x = draw_normal(part_keys[0], (BATCH, D_MODEL), 1.0).astype(jnp.bfloat16)
    w_dq = draw_normal(shared_keys[0], (D_MODEL, Q_LORA), D_MODEL ** -0.5).astype(jnp.bfloat16)
    g_q = jax.random.uniform(shared_keys[1], (Q_LORA,), jnp.float32, 0.5, 1.5)
    w_uq = draw_normal(shared_keys[2], (Q_LORA, HEADS * QK_DIM), Q_LORA ** -0.5).astype(jnp.bfloat16)
    w_dkv = draw_normal(shared_keys[3], (D_MODEL, LATENT + ROPE_DIM), D_MODEL ** -0.5).astype(jnp.bfloat16)
    g_kv = jax.random.uniform(shared_keys[4], (LATENT,), jnp.float32, 0.5, 1.5)
    w_uk = draw_normal(shared_keys[5], (LATENT, HEADS, NOPE_DIM), LATENT ** -0.5).astype(jnp.bfloat16)
    w_uv = draw_normal(shared_keys[6], (LATENT, HEADS, V_DIM), LATENT ** -0.5).astype(jnp.bfloat16)
    w_o = draw_normal(shared_keys[7], (HEADS * V_DIM, D_MODEL), (HEADS * V_DIM) ** -0.5).astype(jnp.bfloat16)
    pos_ramp = 2.0 * jnp.arange(SEQ, dtype=jnp.float32) / SEQ - 1.0
    drift_dir = draw_normal(part_keys[1], (BATCH, 1, LATENT), 1.0)
    cache_c = (draw_normal(part_keys[2], (BATCH, SEQ, LATENT), 1.0) + drift_dir * pos_ramp[None, :, None]).astype(jnp.bfloat16)
    key_base = jnp.broadcast_to(draw_normal(part_keys[3], (BATCH, 1, ROPE_DIM), 1.0), (BATCH, SEQ, ROPE_DIM))
    cos_tab, sin_tab = rope_tables(jnp.arange(SEQ))
    cache_kr = (rope_rotate(key_base, cos_tab[None], sin_tab[None]) + draw_normal(part_keys[4], (BATCH, SEQ, ROPE_DIM), 0.5)).astype(jnp.bfloat16)
    ctx_len = jax.random.randint(part_keys[5], (BATCH,), SEQ // 2, SEQ, dtype=jnp.int32).at[0].set(SEQ - 1)
    return {'x': x, 'w_dq': w_dq, 'g_q': g_q, 'w_uq': w_uq, 'w_dkv': w_dkv, 'g_kv': g_kv, 'w_uk': w_uk, 'w_uv': w_uv, 'w_o': w_o, 'cache_c': cache_c, 'cache_kr': cache_kr, 'ctx_len': ctx_len}


def reference(x, w_dq, g_q, w_uq, w_dkv, g_kv, w_uk, w_uv, w_o, cache_c, cache_kr, ctx_len):
    cq_low = jnp.dot(x, w_dq, preferred_element_type=jnp.float32).astype(jnp.bfloat16)
    cq_norm = rms_norm(cq_low.astype(jnp.float32), g_q).astype(jnp.bfloat16)
    q_full = jnp.dot(cq_norm, w_uq, preferred_element_type=jnp.float32).astype(jnp.bfloat16).reshape(BATCH, HEADS, QK_DIM)
    cos_tab, sin_tab = rope_tables(ctx_len)
    q_rope = rope_rotate(q_full[:, :, NOPE_DIM:].astype(jnp.float32), cos_tab[:, None, :], sin_tab[:, None, :]).astype(jnp.bfloat16)
    q_lat = jnp.einsum('bhn,khn->bhk', q_full[:, :, :NOPE_DIM].astype(jnp.float32), w_uk.astype(jnp.float32)).astype(jnp.bfloat16)
    kv_full = jnp.dot(x, w_dkv, preferred_element_type=jnp.float32)
    c_new = rms_norm(kv_full[:, :LATENT], g_kv).astype(jnp.bfloat16)
    kr_new = rope_rotate(kv_full[:, LATENT:], cos_tab, sin_tab).astype(jnp.bfloat16)
    score_scale = QK_DIM ** -0.5
    positions = jnp.arange(SEQ)

    def attend_one(item_args):
        q_lat_r, q_rope_r, c_rows, kr_rows, c_new_r, kr_new_r, req_len = item_args
        scores = (jnp.dot(q_lat_r, c_rows.T, preferred_element_type=jnp.float32) + jnp.dot(q_rope_r, kr_rows.T, preferred_element_type=jnp.float32)) * score_scale
        scores = jnp.where(positions[None, :] < req_len, scores, -jnp.inf)
        new_score = (jnp.dot(q_lat_r, c_new_r, preferred_element_type=jnp.float32) + jnp.dot(q_rope_r, kr_new_r, preferred_element_type=jnp.float32)) * score_scale
        row_max = jnp.maximum(jnp.max(scores, axis=1), new_score)
        weights = jnp.exp(scores - row_max[:, None])
        new_weight = jnp.exp(new_score - row_max)
        row_sum = jnp.sum(weights, axis=1) + new_weight
        lat_acc = jnp.dot(weights.astype(jnp.bfloat16), c_rows, preferred_element_type=jnp.float32)
        lat_acc = lat_acc + new_weight.astype(jnp.bfloat16).astype(jnp.float32)[:, None] * c_new_r.astype(jnp.float32)[None, :]
        return lat_acc / row_sum[:, None]

    o_lat = lax.map(attend_one, (q_lat, q_rope, cache_c, cache_kr, c_new, kr_new, ctx_len)).astype(jnp.bfloat16)
    o_heads = jnp.einsum('bhk,khv->bhv', o_lat.astype(jnp.float32), w_uv.astype(jnp.float32)).astype(jnp.bfloat16)
    attn_out = jnp.dot(o_heads.reshape(BATCH, HEADS * V_DIM), w_o, preferred_element_type=jnp.float32)
    x_out = (x.astype(jnp.float32) + attn_out).astype(jnp.bfloat16)
    return x_out, c_new, kr_new
```

```python
import functools
import math

import jax
import jax.numpy as jnp
import numpy as np
from jax import lax
from jax.experimental import pallas as pl
from jax.experimental.pallas import tpu as pltpu
from jax.sharding import PartitionSpec as P

NORM_EPS = 1e-6
ROPE_THETA = 10000.0
MASKED = -1e30
FLOOR = -1e29
F32, BF16 = jnp.float32, jnp.bfloat16
MESH = pl.DeviceIdType.MESH
NT = (((1,), (1,)), ((), ()))
LANES = 128


def dot(a, b):
    return jnp.dot(a, b, preferred_element_type=F32)


def dot_nt(a, b):
    return lax.dot_general(a, b, NT, preferred_element_type=F32)


def rounded(v):
    return v.astype(BF16).astype(F32)


def wait_bytes(view, sem):
    pltpu.make_async_copy(view, view, sem).wait()


def step_kernel(dims, x_h, wdq_h, gq_h, wuq_h, wdkv_h, gkv_h, wuk_h, wuv_h, wo_h, cc_h, kr_h, freq_h, ctx_s,
                xo_h, cn_h, krn_h,
                x_v, wdq_v, gq_v, wuq_v, wdkv_v, gkv_v, wuk_v, wuv_v, wo_v, cc_v, kr_v, freq_v, wv_v,
                xf_v, cqp_v, kvp_v, qn_v, q_v, cnf_v, acc_v, pair_v, rs_v, rsr_v, olat_v, po_v, pop_v, pt_v, ptr_v, ag_v,
                xo_v, cno_v, krno_v,
                in_sem, uq_sem, uk_sem, cc_sem, out_sem,
                a_send, a_recv, kv_send, kv_recv, q_send, q_recv, pair_send, pair_recv, rs_send, rs_recv,
                po_send, po_recv, pt_send, pt_recv, ag_send, ag_recv, ag2_send, ag2_recv):
    cp, side = dims
    chips = cp // 2
    inner = 2 * side
    nreq, dmodel = x_v.shape
    kdq, ndq = wdq_v.shape
    latent, half_heads, nope = wuk_v.shape
    heads = 2 * half_heads
    rope = kr_v.shape[1]
    half_rope = rope // 2
    tdev = cc_v.shape[1]
    wide = latent + LANES
    qk = nope + rope
    kdkv = wdkv_v.shape[1]
    slab = 8
    own = heads // cp

    d = lax.axis_index('cp')
    c = lax.rem(d, 2)
    t = d // 2
    oc = 1 - c
    gi = lax.rem(d, inner)
    base = d - gi
    xx = gi // 2
    partner = base + 2 * xx + oc

    def chip_at(r):
        return lax.rem(t + r, chips)

    def local(src, dst, sem):
        cpy = pltpu.make_async_copy(src, dst, sem)
        cpy.start()
        return cpy

    cx = local(x_h, x_v, in_sem.at[0])
    cdq = local(wdq_h.at[pl.ds(pl.multiple_of(c * kdq, kdq), kdq), pl.ds(pl.multiple_of(xx * ndq, LANES), ndq)], wdq_v, in_sem.at[1])
    cdkv = local(wdkv_h.at[:, pl.ds(pl.multiple_of(gi * kdkv, LANES), kdkv)], wdkv_v, in_sem.at[2])
    cgq = local(gq_h, gq_v, in_sem.at[3])
    cgkv = local(gkv_h, gkv_v, in_sem.at[4])
    cfreq = local(freq_h, freq_v, in_sem.at[5])
    nslab = half_heads // slab
    uk = [local(wuk_h.at[:, pl.ds(pl.multiple_of(c * half_heads + s * slab, slab), slab), :],
                wuk_v.at[:, pl.ds(s * slab, slab), :], uk_sem.at[s]) for s in range(nslab)]
    nuq = wuq_v.shape[1] // 768
    uq = [local(wuq_h.at[:, pl.ds(pl.multiple_of(c * nuq * 768 + j * 768, LANES), 768)],
                wuq_v.at[:, pl.ds(j * 768, 768)], uq_sem.at[j]) for j in range(nuq)]
    for b in range(nreq):
        local(cc_h.at[b], cc_v.at[b], cc_sem.at[0, b])
        local(kr_h.at[b], kr_v.at[b], cc_sem.at[1, b])
    head0 = c * half_heads + t * own
    head_slab = head0 // slab
    head_in = head0 - head_slab * slab
    cuv = local(wuv_h.at[:, pl.ds(pl.multiple_of(head_slab * slab, slab), slab), :], wuv_v, in_sem.at[6])
    cwo = local(wo_h.at[pl.ds(pl.multiple_of(head0 * nope, own * nope), own * nope), :], wo_v, in_sem.at[7])

    barrier = pltpu.get_barrier_semaphore()

    def greet(r, _):
        pl.semaphore_signal(barrier, inc=1, device_id={'cp': 2 * chip_at(r) + c}, device_id_type=MESH)
        return 0

    lax.fori_loop(1, chips, greet, 0)
    for i in range(side):
        pl.semaphore_signal(barrier, inc=1, device_id={'cp': base + 2 * i + oc}, device_id_type=MESH)

    cx.wait()
    cdq.wait()
    part = dot(x_v[:, pl.ds(pl.multiple_of(c * kdq, kdq), kdq)], wdq_v[...])
    cqp_v[gi] = part
    pl.semaphore_wait(barrier, chips - 1 + side)

    def to_ring(buf, send, recv):
        def go(r, _):
            peer = lax.rem(gi + r, inner)
            pltpu.make_async_remote_copy(src_ref=buf.at[gi], dst_ref=buf.at[gi], send_sem=send, recv_sem=recv,
                                         device_id={'cp': base + peer}, device_id_type=MESH).start()
            return 0
        lax.fori_loop(1, inner, go, 0)

    to_ring(cqp_v, a_send, a_recv)
    cdkv.wait()
    kvp_v[gi, :, 0:latent + rope] = dot_nt(x_v[:, pl.ds(pl.multiple_of(gi * kdkv, LANES), kdkv)], wdkv_v[...])
    kvp_v[gi, :, latent + rope:] = jnp.zeros((nreq, wide - latent - rope), F32)
    to_ring(kvp_v, kv_send, kv_recv)

    xall = x_v[...].astype(F32)
    for i in range(2):
        xf_v[i] = xall[4 * i:4 * i + 4, :]
    rows = lax.broadcasted_iota(jnp.int32, (nreq, LANES), 0)
    ctx = jnp.zeros((nreq, LANES), jnp.int32)
    for b in range(nreq):
        ctx = jnp.where(rows == b, ctx_s[b], ctx)
    cfreq.wait()
    angles = ctx.astype(F32) * freq_v[...]
    cos_full = jnp.cos(angles)[:, :rope]
    sin_raw = jnp.sin(angles)[:, :rope]
    lane = lax.broadcasted_iota(jnp.int32, (nreq, rope), 1)
    sin_full = jnp.where(lane < half_rope, -sin_raw, sin_raw)

    def rope_rotate(v):
        swapped = jnp.concatenate([v[:, half_rope:], v[:, :half_rope]], axis=1)
        return v * cos_full + swapped * sin_full

    wait_bytes(cqp_v.at[pl.ds(0, inner - 1)], a_recv)
    cols = [cqp_v[2 * i] + cqp_v[2 * i + 1] for i in range(side)]
    cq = rounded(jnp.concatenate(cols, axis=1))
    cgq.wait()
    mean_sq = jnp.mean(cq * cq, axis=1, keepdims=True)
    cn = (cq * lax.rsqrt(mean_sq + NORM_EPS) * gq_v[...]).astype(BF16)
    row0 = c * half_heads * nreq
    zeros_pad = jnp.zeros((nreq, LANES - rope), F32)
    for j in range(nuq):
        uq[j].wait()
        qc = rounded(dot(cn, wuq_v[:, j * 768:(j + 1) * 768]))
        for i in range(768 // qk):
            h = j * (768 // qk) + i
            qn_v[h * nreq:(h + 1) * nreq, :] = qc[:, i * qk:i * qk + nope]
            qr = rounded(rope_rotate(qc[:, i * qk + nope:(i + 1) * qk]))
            r = pl.multiple_of(row0 + h * nreq, nreq)
            q_v[latent // LANES, pl.ds(r, nreq), :] = jnp.concatenate([qr, zeros_pad], axis=1)

    def q_slab_copy(s):
        view = q_v.at[:, pl.ds(pl.multiple_of(row0 + s * slab * nreq, slab * nreq), slab * nreq)]
        return pltpu.make_async_remote_copy(src_ref=view, dst_ref=view, send_sem=q_send.at[s], recv_sem=q_recv.at[s],
                                            device_id={'cp': partner}, device_id_type=MESH)

    for s in range(nslab):
        uk[s].wait()
        for i in range(slab):
            h = s * slab + i
            ql = rounded(dot_nt(qn_v[h * nreq:(h + 1) * nreq, :].astype(BF16), wuk_v[:, h, :]))
            r = pl.multiple_of(row0 + h * nreq, nreq)
            for k in range(latent // LANES):
                q_v[k, pl.ds(r, nreq), :] = ql[:, k * LANES:(k + 1) * LANES]
        q_slab_copy(s).start()

    wait_bytes(kvp_v.at[pl.ds(0, inner - 1)], kv_recv)
    kv = kvp_v[0]
    for i in range(1, inner):
        kv = kv + kvp_v[i]
    kvl = kv[:, :latent]
    cgkv.wait()
    mean_sq = jnp.mean(kvl * kvl, axis=1, keepdims=True)
    c_new = kvl * lax.rsqrt(mean_sq + NORM_EPS) * gkv_v[...]
    kr_new = rope_rotate(kv[:, latent:latent + rope])
    cno_v[...] = c_new.astype(BF16)
    krno_v[...] = kr_new.astype(BF16)
    cnf_v[:, :latent] = rounded(c_new)
    cnf_v[:, latent:] = jnp.concatenate([rounded(kr_new), zeros_pad], axis=1)
    ocn = local(cno_v, cn_h, out_sem.at[0])
    okr = local(krno_v, krn_h, out_sem.at[1])

    for s in range(nslab):
        q_slab_copy(s).wait()

    scale = (nope + rope) ** -0.5
    block0 = d * tdev
    key_pos = lax.broadcasted_iota(jnp.int32, (heads, tdev), 1)
    head_row = lax.broadcasted_iota(jnp.int32, (heads, 1), 0)
    lane1 = lax.broadcasted_iota(jnp.int32, (half_heads, LANES), 1)
    mine0 = pl.multiple_of(c * half_heads, half_heads)
    theirs0 = pl.multiple_of(oc * half_heads, half_heads)

    def pair_copy(b):
        return pltpu.make_async_remote_copy(src_ref=acc_v.at[b, pl.ds(theirs0, half_heads)], dst_ref=pair_v.at[b],
                                            send_sem=pair_send.at[b], recv_sem=pair_recv.at[b],
                                            device_id={'cp': partner}, device_id_type=MESH)

    def attend(b):
        pltpu.make_async_copy(cc_v.at[b], cc_v.at[b], cc_sem.at[0, b]).wait()
        pltpu.make_async_copy(kr_v.at[b], kr_v.at[b], cc_sem.at[1, b]).wait()
        qf = jnp.concatenate([q_v[k, pl.ds(b, heads, stride=nreq), :] for k in range(wide // LANES)], axis=1)
        qb = qf.astype(BF16)
        s = (dot_nt(qb[:, :latent], cc_v[b]) + dot(qb[:, latent:latent + rope], kr_v[b])) * scale
        left = ctx_s[b] - block0
        s = jnp.where(key_pos < left, s, MASKED)
        new_row = cnf_v[pl.ds(b, 1), :]
        new_s = jnp.sum(qf * new_row, axis=1, keepdims=True) * scale
        at = head_row * 0 + left
        owner = jnp.logical_and(at >= 0, at < tdev)
        new_s = jnp.where(owner, new_s, MASKED)
        m = jnp.maximum(jnp.maximum(jnp.max(s, axis=1, keepdims=True), new_s), FLOOR)
        p = jnp.exp(s - m)
        new_w = jnp.exp(new_s - m)
        l = jnp.sum(p, axis=1, keepdims=True) + new_w
        acc = dot(p.astype(BF16), cc_v[b]) + rounded(new_w) * new_row[:, :latent]
        acc_v[b, :, :latent] = acc
        ml_lane = lax.broadcasted_iota(jnp.int32, (heads, LANES), 1)
        acc_v[b, :, latent:] = jnp.where(ml_lane < LANES // 2, m, l)
        pair_copy(b).start()

    def rs_copy(b, r):
        return pltpu.make_async_remote_copy(src_ref=rs_v.at[b, chip_at(r)], dst_ref=rsr_v.at[b, r - 1],
                                            send_sem=rs_send.at[b], recv_sem=rs_recv.at[b],
                                            device_id={'cp': 2 * chip_at(r) + c}, device_id_type=MESH)

    def pair_merge(b):
        pair_copy(b).wait_recv()
        a1 = acc_v[b, pl.ds(mine0, half_heads), :]
        a2 = pair_v[b]
        m1, m2 = a1[:, latent:latent + 1], a2[:, latent:latent + 1]
        l1, l2 = a1[:, wide - 1:wide], a2[:, wide - 1:wide]
        m = jnp.maximum(m1, m2)
        f1, f2 = jnp.exp(m1 - m), jnp.exp(m2 - m)
        acc = f1 * a1[:, :latent] + f2 * a2[:, :latent]
        ml = jnp.where(lane1 < LANES // 2, m, f1 * l1 + f2 * l2)
        for k in range(chips):
            rs_v[b, k, :, :latent] = acc[own * k:own * (k + 1), :]
            rs_v[b, k, :, latent:] = ml[own * k:own * (k + 1), :]

        def go(r, _):
            rs_copy(b, r).start()
            return 0
        lax.fori_loop(1, chips, go, 0)

    def attend_step(b, _):
        attend(b)

        @pl.when(b > 0)
        def _():
            pair_merge(b - 1)
        return 0

    lax.fori_loop(0, nreq, attend_step, 0)
    pair_merge(nreq - 1)

    cuv.wait()
    for i in range(slab // own):
        @pl.when(head_in == i * own)
        def _():
            for k in range(own):
                wv_v[k] = wuv_v[:, i * own + k, :]

    def owner_merge(b, _):
        wait_bytes(rsr_v.at[b], rs_recv.at[b])
        first = rs_v[b, t]
        rest = rsr_v[b]
        m0, l0 = first[:, latent:latent + 1], first[:, wide - 1:wide]
        mr, lr = rest[:, :, latent:latent + 1], rest[:, :, wide - 1:wide]
        m = jnp.maximum(jnp.max(mr, axis=0), m0)
        f0, fr = jnp.exp(m0 - m), jnp.exp(mr - m[None])
        l = f0 * l0 + jnp.sum(fr * lr, axis=0)
        acc = f0 * first[:, :latent] + jnp.sum(fr * rest[:, :, :latent], axis=0)
        ol = rounded(acc / l)
        for k in range(own):
            olat_v[k, pl.ds(b, 1), :] = ol[k:k + 1, :]
        return 0

    lax.fori_loop(0, nreq, owner_merge, 0)

    cwo.wait()
    outs = []
    for k in range(own):
        outs.append(dot(olat_v[k].astype(BF16), wv_v[k]).astype(BF16))
    o = jnp.concatenate(outs, axis=1)
    ncol = 768
    for j in range(dmodel // ncol):
        pj = dot(o, wo_v[:, j * ncol:(j + 1) * ncol])
        for i in range(2):
            po_v[i, :, j * ncol:(j + 1) * ncol] = pj[4 * i:4 * i + 4, :]
    po_copy = pltpu.make_async_remote_copy(src_ref=po_v.at[oc], dst_ref=pop_v, send_sem=po_send, recv_sem=po_recv,
                                           device_id={'cp': partner}, device_id_type=MESH)
    po_copy.start()
    po_copy.wait()
    tcol = dmodel // chips
    for k in range(chips):
        pt_v[k] = po_v[c, :, k * tcol:(k + 1) * tcol] + pop_v[:, k * tcol:(k + 1) * tcol]

    def pt_go(r, _):
        pltpu.make_async_remote_copy(src_ref=pt_v.at[chip_at(r)], dst_ref=ptr_v.at[r - 1], send_sem=pt_send, recv_sem=pt_recv,
                                     device_id={'cp': 2 * chip_at(r) + c}, device_id_type=MESH).start()
        return 0
    lax.fori_loop(1, chips, pt_go, 0)
    wait_bytes(ptr_v, pt_recv)
    tot = pt_v[t]
    for r in range(chips - 1):
        tot = tot + ptr_v[r]
    ag_v[c, t] = rounded(xf_v[c, :, pl.ds(pl.multiple_of(t * tcol, LANES), tcol)] + tot)

    def ag_go(r, _):
        pltpu.make_async_remote_copy(src_ref=ag_v.at[c, t], dst_ref=ag_v.at[c, t], send_sem=ag_send, recv_sem=ag_recv,
                                     device_id={'cp': 2 * chip_at(r) + c}, device_id_type=MESH).start()
        return 0
    lax.fori_loop(1, chips, ag_go, 0)
    wait_bytes(ag_v.at[0, pl.ds(0, chips - 1)], ag_recv)
    ag_copy = pltpu.make_async_remote_copy(src_ref=ag_v.at[c], dst_ref=ag_v.at[c], send_sem=ag2_send, recv_sem=ag2_recv,
                                           device_id={'cp': partner}, device_id_type=MESH)
    ag_copy.start()
    ag_copy.wait()
    for k in range(chips):
        xo_v[:, k * tcol:(k + 1) * tcol] = jnp.concatenate([ag_v[0, k], ag_v[1, k]], axis=0).astype(BF16)
    oxo = local(xo_v, xo_h, out_sem.at[2])

    wait_bytes(cqp_v.at[pl.ds(0, inner - 1)], a_send)
    wait_bytes(kvp_v.at[pl.ds(0, inner - 1)], kv_send)
    wait_bytes(ptr_v, pt_send)
    wait_bytes(ag_v.at[0, pl.ds(0, chips - 1)], ag_send)

    def drain(b, _):
        pair_copy(b).wait_send()
        wait_bytes(rsr_v.at[b], rs_send.at[b])
        return 0
    lax.fori_loop(0, nreq, drain, 0)
    ocn.wait()
    okr.wait()
    oxo.wait()


def solution(mesh):
    cp = mesh.shape['cp']
    side = math.isqrt(cp // 2)
    inner = 2 * side
    chips = cp // 2

    def decode_step(x, w_dq, g_q, w_uq, w_dkv, g_kv, w_uk, w_uv, w_o, cache_c, cache_kr, ctx_len):
        nreq, dmodel = x.shape
        qlora = w_dq.shape[1]
        latent, heads, nope = w_uk.shape
        rope = cache_kr.shape[2]
        tdev = cache_c.shape[1]
        half = heads // 2
        own = heads // cp
        wide = latent + LANES
        tcol = dmodel // chips
        inv = (np.float64(ROPE_THETA) ** (-2.0 * np.arange(rope // 2) / rope)).astype(np.float32)
        freq = np.zeros((1, LANES), np.float32)
        freq[0, :rope] = np.concatenate([inv, inv])
        anyspec = pl.BlockSpec(memory_space=pl.ANY)
        dma = pltpu.SemaphoreType.DMA
        vm = pltpu.VMEM
        out_shape = (jax.ShapeDtypeStruct((nreq, dmodel), BF16), jax.ShapeDtypeStruct((nreq, latent), BF16),
                     jax.ShapeDtypeStruct((nreq, rope), BF16))
        scratch = [
            vm((nreq, dmodel), BF16), vm((dmodel // 2, qlora // side), BF16), vm((1, qlora), F32),
            vm((qlora, w_uq.shape[1] // 2), BF16), vm((w_dkv.shape[1], dmodel // inner), BF16), vm((1, latent), F32),
            vm((latent, half, nope), BF16), vm((latent, 8, nope), BF16), vm((own * nope, dmodel), BF16),
            vm((nreq, tdev, latent), BF16), vm((nreq, rope, tdev), BF16), vm((1, LANES), F32), vm((own, latent, nope), BF16),
            vm((2, nreq // 2, dmodel), F32), vm((inner, nreq, qlora // side), F32), vm((inner, nreq, wide), F32),
            vm((half * nreq, nope), F32), vm((wide // LANES, heads * nreq, LANES), F32), vm((nreq, wide), F32),
            vm((nreq, heads, wide), F32), vm((nreq, half, wide), F32),
            vm((nreq, chips, own, wide), F32), vm((nreq, chips - 1, own, wide), F32), vm((own, nreq, latent), F32),
            vm((2, nreq // 2, dmodel), F32), vm((nreq // 2, dmodel), F32),
            vm((chips, nreq // 2, tcol), F32), vm((chips - 1, nreq // 2, tcol), F32), vm((2, chips, nreq // 2, tcol), F32),
            vm((nreq, dmodel), BF16), vm((nreq, latent), BF16), vm((nreq, rope), BF16),
            dma((8,)), dma((w_uq.shape[1] // 2 // 768,)), dma((half // 8,)), dma((2, nreq)), dma((3,)),
            dma, dma, dma, dma, dma((half // 8,)), dma((half // 8,)), dma((nreq,)), dma((nreq,)), dma((nreq,)), dma((nreq,)),
            dma, dma, dma, dma, dma, dma, dma, dma,
        ]
        return pl.pallas_call(
            functools.partial(step_kernel, (cp, side)),
            out_shape=out_shape,
            in_specs=[anyspec] * 12 + [pl.BlockSpec(memory_space=pltpu.SMEM)],
            out_specs=(anyspec,) * 3,
            scratch_shapes=scratch,
            compiler_params=pltpu.CompilerParams(collective_id=0, has_side_effects=True, vmem_limit_bytes=67043328),
            name='decode_step',
        )(x, w_dq, g_q.reshape(1, qlora), w_uq, w_dkv.T, g_kv.reshape(1, latent), w_uk, w_uv, w_o,
          cache_c, jnp.swapaxes(cache_kr, 1, 2), jnp.asarray(freq), ctx_len)

    spec_rows = P('dp', None)
    spec_cache = P('dp', 'cp', None)
    in_specs = (spec_rows, P(), P(), P(), P(), P(), P(), P(), P(), spec_cache, spec_cache, P('dp'))
    out_specs = (spec_rows, spec_rows, spec_rows)
    return jax.shard_map(decode_step, mesh=mesh, in_specs=in_specs, out_specs=out_specs, check_vma=False)
```

```python
import functools
import math

import jax
import jax.numpy as jnp
import numpy as np
from jax import lax
from jax.experimental import pallas as pl
from jax.experimental.pallas import tpu as pltpu
from jax.sharding import PartitionSpec as P

NORM_EPS = 1e-6
ROPE_THETA = 10000.0
MASKED = -1e30
FLOOR = -1e29
F32, BF16 = jnp.float32, jnp.bfloat16
MESH = pl.DeviceIdType.MESH
NT = (((1,), (1,)), ((), ()))
LANES = 128


def dot(a, b):
    return jnp.dot(a, b, preferred_element_type=F32)


def dot_nt(a, b):
    return lax.dot_general(a, b, NT, preferred_element_type=F32)


def rounded(v):
    return v.astype(BF16).astype(F32)


def wait_bytes(view, sem):
    pltpu.make_async_copy(view, view, sem).wait()


def step_kernel(dims, x_h, wdq_h, gq_h, wuq_h, wdkv_h, gkv_h, wuk_h, wuv_h, wo_h, cc_h, kr_h, freq_h, ctx_s,
                out_v,
                x_v, wdq_v, gq_v, wuq_v, wdkv_v, gkv_v, wuk_v, wuv_v, wo_v, cc_v, kr_v, freq_v, wv_v, wk_v, stage_v,
                xf_v, cqp_v, kvp_v, q_v, cnf_v, acc_v, pair_v, xs_v, xsr_v, ys_v, ysr_v, olat_v, po_v, pop_v, pt_v, ptr_v, ag_v,
                in_sem, uq_sem, uk_sem, cc_sem,
                a_send, a_recv, kv_send, kv_recv, q_send, q_recv, pair_send, pair_recv, xs_send, xs_recv, ys_send, ys_recv,
                po_send, po_recv, pt_send, pt_recv, ag_send, ag_recv, ag2_send, ag2_recv):
    cp, side = dims
    chips = cp // 2
    inner = 2 * side
    nreq, dmodel = x_v.shape
    kdq, ndq = wdq_v.shape
    nslab, latent, slab, nope = wuk_v.shape
    half_heads = nslab * slab
    heads = 2 * half_heads
    rope = kr_v.shape[1]
    half_rope = rope // 2
    tdev = cc_v.shape[1]
    wide = latent + LANES
    qk = nope + rope
    kdkv = wdkv_v.shape[1]
    own = heads // cp

    d = lax.axis_index('cp')
    c = lax.rem(d, 2)
    t = d // 2
    oc = 1 - c
    gi = lax.rem(d, inner)
    base = d - gi
    xx = gi // 2
    yy = d // inner
    partner = base + 2 * xx + oc

    kstep = 64

    def widen(src):
        def go(i, _):
            r = pl.multiple_of(i * kstep, kstep)
            stage_v[pl.ds(pl.multiple_of(r * slab, kstep * slab), kstep * slab), :] = (
                src[pl.ds(r, kstep)].astype(F32).reshape(kstep * slab, nope))
            return 0
        lax.fori_loop(0, latent // kstep, go, 0)

    def chip_at(r):
        return lax.rem(t + r, chips)

    pending = {}

    def done(name):
        pending.pop(name)()

    def drain():
        for name in list(pending):
            done(name)

    def local(name, src, dst, sem):
        cpy = pltpu.make_async_copy(src, dst, sem)
        cpy.start()
        pending[name] = cpy.wait

    later = []

    def issue(n):
        for _ in range(min(n, len(later))):
            for args in later.pop(0):
                local(*args)

    local('x', x_h, x_v, in_sem.at[0])
    local('dq', wdq_h.at[pl.ds(pl.multiple_of(c * kdq, kdq), kdq), pl.ds(pl.multiple_of(xx * ndq, LANES), ndq)], wdq_v, in_sem.at[1])
    local('dkv', wdkv_h.at[:, pl.ds(pl.multiple_of(gi * kdkv, LANES), kdkv)], wdkv_v, in_sem.at[2])
    local('gq', gq_h, gq_v, in_sem.at[3])
    local('gkv', gkv_h, gkv_v, in_sem.at[4])
    local('freq', freq_h, freq_v, in_sem.at[5])
    ucol = 768
    nuq = wuq_v.shape[1] // ucol
    for s in range(nslab):
        local(('uk', s), wuk_h.at[:, pl.ds(pl.multiple_of(c * half_heads + s * slab, slab), slab), :], wuk_v.at[s], uk_sem.at[s])
    for j in range(nuq):
        later.append([(('uq', j), wuq_h.at[:, pl.ds(pl.multiple_of(c * nuq * ucol + j * ucol, LANES), ucol)],
                       wuq_v.at[:, pl.ds(j * ucol, ucol)], uq_sem.at[j])])
    for b in range(nreq):
        later.append([(('cc', b), cc_h.at[b], cc_v.at[b], cc_sem.at[0, b]), (('kr', b), kr_h.at[b], kr_v.at[b], cc_sem.at[1, b])])
    head0 = c * half_heads + xx * slab + yy * own
    head_slab = head0 // slab
    head_in = head0 - head_slab * slab
    later.append([('uv', wuv_h.at[:, pl.ds(pl.multiple_of(head_slab * slab, slab), slab), :], wuv_v, in_sem.at[6])])
    later.append([('wo', wo_h.at[pl.ds(pl.multiple_of(head0 * nope, own * nope), own * nope), :], wo_v, in_sem.at[7])])

    barrier = pltpu.get_barrier_semaphore()

    def greet(r, _):
        pl.semaphore_signal(barrier, inc=1, device_id={'cp': 2 * chip_at(r) + c}, device_id_type=MESH)
        return 0

    lax.fori_loop(1, chips, greet, 0)
    for i in range(side):
        pl.semaphore_signal(barrier, inc=1, device_id={'cp': base + 2 * i + oc}, device_id_type=MESH)

    done('x')
    done('dq')
    part = dot(x_v[:, pl.ds(pl.multiple_of(c * kdq, kdq), kdq)], wdq_v[...])
    cqp_v[gi] = part
    issue(2)
    pl.semaphore_wait(barrier, chips - 1 + side)

    def to_ring(buf, send, recv):
        def go(r, _):
            peer = lax.rem(gi + r, inner)
            pltpu.make_async_remote_copy(src_ref=buf.at[gi], dst_ref=buf.at[gi], send_sem=send, recv_sem=recv,
                                         device_id={'cp': base + peer}, device_id_type=MESH).start()
            return 0
        lax.fori_loop(1, inner, go, 0)

    to_ring(cqp_v, a_send, a_recv)
    issue(1)
    pending['a_send'] = lambda: wait_bytes(cqp_v.at[pl.ds(0, inner - 1)], a_send)
    pending['a_recv'] = lambda: wait_bytes(cqp_v.at[pl.ds(0, inner - 1)], a_recv)
    done('dkv')
    kvp_v[gi, :, 0:latent + rope] = dot_nt(x_v[:, pl.ds(pl.multiple_of(gi * kdkv, LANES), kdkv)], wdkv_v[...])
    kvp_v[gi, :, latent + rope:] = jnp.zeros((nreq, wide - latent - rope), F32)
    to_ring(kvp_v, kv_send, kv_recv)
    pending['kv_send'] = lambda: wait_bytes(kvp_v.at[pl.ds(0, inner - 1)], kv_send)
    pending['kv_recv'] = lambda: wait_bytes(kvp_v.at[pl.ds(0, inner - 1)], kv_recv)

    issue(1)

    xall = x_v[...].astype(F32)
    for i in range(2):
        xf_v[i] = xall[4 * i:4 * i + 4, :]
    rows = lax.broadcasted_iota(jnp.int32, (nreq, LANES), 0)
    ctx = jnp.zeros((nreq, LANES), jnp.int32)
    for b in range(nreq):
        ctx = jnp.where(rows == b, ctx_s[b], ctx)
    done('freq')
    angles = ctx.astype(F32) * freq_v[...]
    cos_full = jnp.cos(angles)[:, :rope]
    sin_raw = jnp.sin(angles)[:, :rope]
    lane = lax.broadcasted_iota(jnp.int32, (nreq, rope), 1)
    sin_full = jnp.where(lane < half_rope, -sin_raw, sin_raw)

    def rope_rotate(v):
        swapped = jnp.concatenate([v[:, half_rope:], v[:, :half_rope]], axis=1)
        return v * cos_full + swapped * sin_full

    for s in range(nslab):
        done(('uk', s))
        issue(1)
        widen(wuk_v.at[s])
        for i in range(slab):
            wk_v[s * slab + i] = stage_v[pl.ds(i, latent, stride=slab), :].astype(BF16)

    done('a_recv')
    cols = [cqp_v[2 * i] + cqp_v[2 * i + 1] for i in range(side)]
    cq = rounded(jnp.concatenate(cols, axis=1))
    done('gq')
    mean_sq = jnp.mean(cq * cq, axis=1, keepdims=True)
    cn = (cq * lax.rsqrt(mean_sq + NORM_EPS) * gq_v[...].reshape(1, gq_v.shape[0])).astype(BF16)
    row0 = c * half_heads * nreq
    zeros_pad = jnp.zeros((nreq, LANES - rope), F32)
    per = ucol // qk

    def q_slab_copy(s):
        view = q_v.at[:, pl.ds(pl.multiple_of(row0 + s * slab * nreq, slab * nreq), slab * nreq)]
        return pltpu.make_async_remote_copy(src_ref=view, dst_ref=view, send_sem=q_send.at[s], recv_sem=q_recv.at[s],
                                            device_id={'cp': partner}, device_id_type=MESH)

    for j in range(nuq):
        done(('uq', j))
        issue(1)
        qc = rounded(dot(cn, wuq_v[:, j * ucol:(j + 1) * ucol]))
        for i in range(per):
            h = j * per + i
            r = pl.multiple_of(row0 + h * nreq, nreq)
            qr = rounded(rope_rotate(qc[:, i * qk + nope:(i + 1) * qk]))
            q_v[latent // LANES, pl.ds(r, nreq), :] = jnp.concatenate([qr, zeros_pad], axis=1)
            ql = rounded(dot_nt(qc[:, i * qk:i * qk + nope].astype(BF16), wk_v[h]))
            for k in range(latent // LANES):
                q_v[k, pl.ds(r, nreq), :] = ql[:, k * LANES:(k + 1) * LANES]
        if (j + 1) * per % slab == 0:
            s = (j + 1) * per // slab - 1
            q_slab_copy(s).start()
            pending['q', s] = q_slab_copy(s).wait

    issue(len(later))

    done('kv_recv')
    kv = kvp_v[0]
    for i in range(1, inner):
        kv = kv + kvp_v[i]
    kvl = kv[:, :latent]
    done('gkv')
    mean_sq = jnp.mean(kvl * kvl, axis=1, keepdims=True)
    c_new = kvl * lax.rsqrt(mean_sq + NORM_EPS) * gkv_v[...]
    kr_new = rope_rotate(kv[:, latent:latent + rope])
    out_v[:, dmodel:dmodel + latent] = c_new.astype(BF16)
    out_v[:, dmodel + latent:] = jnp.concatenate([kr_new, zeros_pad], axis=1).astype(BF16)
    cnf_v[:, :latent] = rounded(c_new)
    cnf_v[:, latent:] = jnp.concatenate([rounded(kr_new), zeros_pad], axis=1)

    for s in range(nslab):
        done(('q', s))

    scale = (nope + rope) ** -0.5
    block0 = d * tdev
    key_pos = lax.broadcasted_iota(jnp.int32, (heads, tdev), 1)
    head_row = lax.broadcasted_iota(jnp.int32, (heads, 1), 0)
    mine0 = pl.multiple_of(c * half_heads, half_heads)
    theirs0 = pl.multiple_of(oc * half_heads, half_heads)

    def pair_copy(b):
        return pltpu.make_async_remote_copy(src_ref=acc_v.at[b, pl.ds(theirs0, half_heads)], dst_ref=pair_v.at[b],
                                            send_sem=pair_send.at[b], recv_sem=pair_recv.at[b],
                                            device_id={'cp': partner}, device_id_type=MESH)

    def attend(b):
        pltpu.make_async_copy(cc_v.at[b], cc_v.at[b], cc_sem.at[0, b]).wait()
        pltpu.make_async_copy(kr_v.at[b], kr_v.at[b], cc_sem.at[1, b]).wait()
        qf = jnp.concatenate([q_v[k, pl.ds(b, heads, stride=nreq), :] for k in range(wide // LANES)], axis=1)
        qb = qf.astype(BF16)
        s = (dot_nt(qb[:, :latent], cc_v[b]) + dot(qb[:, latent:latent + rope], kr_v[b])) * scale
        left = ctx_s[b] - block0
        s = jnp.where(key_pos < left, s, MASKED)
        new_row = cnf_v[pl.ds(b, 1), :]
        new_s = jnp.sum(qf * new_row, axis=1, keepdims=True) * scale
        at = head_row * 0 + left
        owner = jnp.logical_and(at >= 0, at < tdev)
        new_s = jnp.where(owner, new_s, MASKED)
        m = jnp.maximum(jnp.maximum(jnp.max(s, axis=1, keepdims=True), new_s), FLOOR)
        p = jnp.exp(s - m)
        new_w = jnp.exp(new_s - m)
        l = jnp.sum(p, axis=1, keepdims=True) + new_w
        acc = dot(p.astype(BF16), cc_v[b]) + rounded(new_w) * new_row[:, :latent]
        acc_v[b, :, :latent] = acc
        ml_lane = lax.broadcasted_iota(jnp.int32, (heads, LANES), 1)
        acc_v[b, :, latent:] = jnp.where(ml_lane < LANES // 2, m, l)
        pair_copy(b).start()

    quarter = half_heads // side

    def xs_copy(b, r):
        px = lax.rem(xx + r, side)
        return pltpu.make_async_remote_copy(src_ref=xs_v.at[b, pl.ds(pl.multiple_of(px * quarter, quarter), quarter)],
                                            dst_ref=xsr_v.at[b, r - 1], send_sem=xs_send.at[b], recv_sem=xs_recv.at[b],
                                            device_id={'cp': base + 2 * px + c}, device_id_type=MESH)

    def ys_copy(b, r):
        py = lax.rem(yy + r, side)
        return pltpu.make_async_remote_copy(src_ref=ys_v.at[b, py], dst_ref=ysr_v.at[b, r - 1],
                                            send_sem=ys_send.at[b], recv_sem=ys_recv.at[b],
                                            device_id={'cp': py * inner + gi}, device_id_type=MESH)

    def ml_of(v):
        return v[:, latent:latent + 1], v[:, wide - 1:wide]

    def merge(parts):
        ms, ls = zip(*[ml_of(p) for p in parts])
        m = functools.reduce(jnp.maximum, ms)
        fs = [jnp.exp(mi - m) for mi in ms]
        l = sum(f * li for f, li in zip(fs, ls))
        acc = sum(f * p[:, :latent] for f, p in zip(fs, parts))
        return m, l, acc

    def with_ml(m, l):
        side_lane = lax.broadcasted_iota(jnp.int32, (m.shape[0], LANES), 1)
        return jnp.where(side_lane < LANES // 2, m, l)

    def pair_merge(b):
        pair_copy(b).wait_recv()
        m, l, acc = merge([acc_v[b, pl.ds(mine0, half_heads), :], pair_v[b]])
        xs_v[b, :, :latent] = acc
        xs_v[b, :, latent:] = with_ml(m, l)
        for r in range(1, side):
            xs_copy(b, r).start()

    def ring_merge(b):
        wait_bytes(xsr_v.at[b], xs_recv.at[b])
        mine = xs_v[b, pl.ds(pl.multiple_of(xx * quarter, quarter), quarter), :]
        m, l, acc = merge([mine] + [xsr_v[b, r] for r in range(side - 1)])
        ml = with_ml(m, l)
        for k in range(side):
            ys_v[b, k, :, :latent] = acc[own * k:own * (k + 1), :]
            ys_v[b, k, :, latent:] = ml[own * k:own * (k + 1), :]
        for r in range(1, side):
            ys_copy(b, r).start()

    lag = 4

    def attend_step(b, _):
        attend(b)

        @pl.when(b > 0)
        def _():
            pair_merge(b - 1)

        @pl.when(b >= lag)
        def _():
            ring_merge(b - lag)
        return 0

    lax.fori_loop(0, nreq, attend_step, 0)
    for b in range(nreq):
        pending.pop(('cc', b))
        pending.pop(('kr', b))
        pending['pair', b] = pair_copy(b).wait_send
    pair_merge(nreq - 1)

    def ring_step(b, _):
        ring_merge(b)
        return 0

    lax.fori_loop(nreq - lag, nreq, ring_step, 0)

    def each(view, sem):
        def go(b, _):
            wait_bytes(view.at[b], sem.at[b])
            return 0
        return lambda: lax.fori_loop(0, nreq, go, 0)

    pending['xs_send'] = each(xsr_v, xs_send)
    pending['ys_send'] = each(ysr_v, ys_send)
    pending['ys_recv'] = each(ysr_v, ys_recv)

    done('uv')
    widen(wuv_v)
    for k in range(own):
        wv_v[k] = stage_v[pl.ds(head_in + k, latent, stride=slab), :].astype(BF16)

    def owner_merge(b, _):
        wait_bytes(ysr_v.at[b], ys_recv.at[b])
        m, l, acc = merge([ys_v[b, yy]] + [ysr_v[b, r] for r in range(side - 1)])
        ol = rounded(acc / l)
        for k in range(own):
            olat_v[k, pl.ds(b, 1), :] = ol[k:k + 1, :]
        return 0

    lax.fori_loop(0, nreq, owner_merge, 0)
    pending.pop('ys_recv')

    done('wo')
    outs = []
    for k in range(own):
        outs.append(dot(olat_v[k].astype(BF16), wv_v[k]).astype(BF16))
    o = jnp.concatenate(outs, axis=1)
    ncol = 768
    for j in range(dmodel // ncol):
        pj = dot(o, wo_v[:, j * ncol:(j + 1) * ncol])
        for i in range(2):
            po_v[i, :, j * ncol:(j + 1) * ncol] = pj[4 * i:4 * i + 4, :]
    po_copy = pltpu.make_async_remote_copy(src_ref=po_v.at[oc], dst_ref=pop_v, send_sem=po_send, recv_sem=po_recv,
                                           device_id={'cp': partner}, device_id_type=MESH)
    po_copy.start()
    po_copy.wait()
    tcol = dmodel // chips
    for k in range(chips):
        pt_v[k] = po_v[c, :, k * tcol:(k + 1) * tcol] + pop_v[:, k * tcol:(k + 1) * tcol]

    def pt_go(r, _):
        pltpu.make_async_remote_copy(src_ref=pt_v.at[chip_at(r)], dst_ref=ptr_v.at[r - 1], send_sem=pt_send, recv_sem=pt_recv,
                                     device_id={'cp': 2 * chip_at(r) + c}, device_id_type=MESH).start()
        return 0
    lax.fori_loop(1, chips, pt_go, 0)
    pending['pt_send'] = lambda: wait_bytes(ptr_v, pt_send)
    wait_bytes(ptr_v, pt_recv)
    tot = pt_v[t]
    for r in range(chips - 1):
        tot = tot + ptr_v[r]
    ag_v[c, t] = rounded(xf_v[c, :, pl.ds(pl.multiple_of(t * tcol, LANES), tcol)] + tot)

    def ag_go(r, _):
        pltpu.make_async_remote_copy(src_ref=ag_v.at[c, t], dst_ref=ag_v.at[c, t], send_sem=ag_send, recv_sem=ag_recv,
                                     device_id={'cp': 2 * chip_at(r) + c}, device_id_type=MESH).start()
        return 0
    lax.fori_loop(1, chips, ag_go, 0)
    pending['ag_send'] = lambda: wait_bytes(ag_v.at[0, pl.ds(0, chips - 1)], ag_send)
    wait_bytes(ag_v.at[0, pl.ds(0, chips - 1)], ag_recv)
    ag_copy = pltpu.make_async_remote_copy(src_ref=ag_v.at[c], dst_ref=ag_v.at[c], send_sem=ag2_send, recv_sem=ag2_recv,
                                           device_id={'cp': partner}, device_id_type=MESH)
    ag_copy.start()
    ag_copy.wait()
    for k in range(chips):
        out_v[:, k * tcol:(k + 1) * tcol] = jnp.concatenate([ag_v[0, k], ag_v[1, k]], axis=0).astype(BF16)

    drain()


def split_outputs(packed_v, xo_v, cn_v, kr_v):
    dmodel, latent, rope = xo_v.shape[1], cn_v.shape[1], kr_v.shape[1]
    xo_v[...] = packed_v[:, :dmodel]
    cn_v[...] = packed_v[:, dmodel:dmodel + latent]
    kr_v[...] = packed_v[:, dmodel + latent:dmodel + latent + rope]


def solution(mesh):
    cp = mesh.shape['cp']
    side = math.isqrt(cp // 2)
    inner = 2 * side
    chips = cp // 2

    def decode_step(x, w_dq, g_q, w_uq, w_dkv, g_kv, w_uk, w_uv, w_o, cache_c, cache_kr, ctx_len):
        nreq, dmodel = x.shape
        qlora = w_dq.shape[1]
        latent, heads, nope = w_uk.shape
        rope = cache_kr.shape[2]
        tdev = cache_c.shape[1]
        half = heads // 2
        own = heads // cp
        wide = latent + LANES
        tcol = dmodel // chips
        inv = (np.float64(ROPE_THETA) ** (-2.0 * np.arange(rope // 2) / rope)).astype(np.float32)
        freq = np.zeros((1, LANES), np.float32)
        freq[0, :rope] = np.concatenate([inv, inv])
        anyspec = pl.BlockSpec(memory_space=pl.ANY)
        dma = pltpu.SemaphoreType.DMA
        vm = pltpu.VMEM
        out_shape = (jax.ShapeDtypeStruct((nreq, dmodel), BF16), jax.ShapeDtypeStruct((nreq, latent), BF16),
                     jax.ShapeDtypeStruct((nreq, rope), BF16))
        scratch = [
            vm((nreq, dmodel), BF16), vm((dmodel // 2, qlora // side), BF16), vm((qlora,), F32),
            vm((qlora, w_uq.shape[1] // 2), BF16), vm((w_dkv.shape[1], dmodel // inner), BF16), vm((1, latent), F32),
            vm((half // 8, latent, 8, nope), BF16), vm((latent, 8, nope), BF16), vm((own * nope, dmodel), BF16),
            vm((nreq, tdev, latent), BF16), vm((nreq, rope, tdev), BF16), vm((1, LANES), F32), vm((own, latent, nope), BF16),
            vm((half, latent, nope), BF16), vm((latent * 8, nope), F32),
            vm((2, nreq // 2, dmodel), F32), vm((inner, nreq, qlora // side), F32), vm((inner, nreq, wide), F32),
            vm((wide // LANES, heads * nreq, LANES), F32), vm((nreq, wide), F32),
            vm((nreq, heads, wide), F32), vm((nreq, half, wide), F32),
            vm((nreq, half, wide), F32), vm((nreq, side - 1, half // side, wide), F32),
            vm((nreq, side, own, wide), F32), vm((nreq, side - 1, own, wide), F32), vm((own, nreq, latent), F32),
            vm((2, nreq // 2, dmodel), F32), vm((nreq // 2, dmodel), F32),
            vm((chips, nreq // 2, tcol), F32), vm((chips - 1, nreq // 2, tcol), F32), vm((2, chips, nreq // 2, tcol), F32),
            dma((8,)), dma((w_uq.shape[1] // 2 // 768,)), dma((half // 8,)), dma((2, nreq)),
            dma, dma, dma, dma, dma((half // 8,)), dma((half // 8,)), dma((nreq,)), dma((nreq,)), dma((nreq,)), dma((nreq,)), dma((nreq,)), dma((nreq,)),
            dma, dma, dma, dma, dma, dma, dma, dma,
        ]
        packed = pl.pallas_call(
            functools.partial(step_kernel, (cp, side)),
            out_shape=jax.ShapeDtypeStruct((nreq, dmodel + wide), BF16),
            in_specs=[anyspec] * 12 + [pl.BlockSpec(memory_space=pltpu.SMEM)],
            out_specs=pl.BlockSpec(memory_space=pltpu.VMEM),
            scratch_shapes=scratch,
            compiler_params=pltpu.CompilerParams(collective_id=0, has_side_effects=True, vmem_limit_bytes=67043328),
            name='decode_step',
        )(x, w_dq, g_q, w_uq, w_dkv.T, g_kv.reshape(1, latent), w_uk, w_uv, w_o,
          cache_c, jnp.swapaxes(cache_kr, 1, 2), jnp.asarray(freq), ctx_len)
        vspec = pl.BlockSpec(memory_space=pltpu.VMEM)
        return pl.pallas_call(split_outputs, out_shape=out_shape, in_specs=[vspec], out_specs=(vspec,) * 3,
                              name='split_outputs')(packed)

    spec_rows = P('dp', None)
    spec_cache = P('dp', 'cp', None)
    in_specs = (spec_rows, P(), P(), P(), P(), P(), P(), P(), P(), spec_cache, spec_cache, P('dp'))
    out_specs = (spec_rows, spec_rows, spec_rows)
    return jax.shard_map(decode_step, mesh=mesh, in_specs=in_specs, out_specs=out_specs, check_vma=False)
```

```python
import functools
import math

import jax
import jax.numpy as jnp
import numpy as np
from jax import lax
from jax.experimental import pallas as pl
from jax.experimental.pallas import tpu as pltpu
from jax.sharding import PartitionSpec as P

NORM_EPS = 1e-6
ROPE_THETA = 10000.0
MASKED = -1e30
FLOOR = -1e29
F32, BF16 = jnp.float32, jnp.bfloat16
MESH = pl.DeviceIdType.MESH
NT = (((1,), (1,)), ((), ()))
LANES = 128


def dot(a, b):
    return jnp.dot(a, b, preferred_element_type=F32)


def dot_nt(a, b):
    return lax.dot_general(a, b, NT, preferred_element_type=F32)


def rounded(v):
    return v.astype(BF16).astype(F32)


def wait_bytes(view, sem):
    pltpu.make_async_copy(view, view, sem).wait()


def step_kernel(dims, x_h, wdq_h, gq_h, wuq_h, wdkv_h, gkv_h, wuk_h, wuv_h, wo_h, cc_h, kr_h, freq_h, ctx_s,
                out_v,
                x_v, gq_v, wuq_v, wdkv_v, gkv_v, wuk_v, wuv_v, wo_v, cc_v, kr_v, freq_v, wv_v, wk_v, stage_v,
                xf_v, cq_v, kvp_v, q_v, cnf_v, sa_v, sb_v, m_v, acc_v, pair_v, xs_v, xsr_v, ys_v, ysr_v, olat_v, po_v, pop_v, pt_v, ptr_v, ag_v,
                in_sem, dq_sem, uq_sem, uk_sem, cc_sem,
                a_send, a_recv, kv_send, kv_recv, q_send, q_recv, pair_send, pair_recv, xs_send, xs_recv, ys_send, ys_recv,
                po_send, po_recv, pt_send, pt_recv, ag_send, ag_recv, ag2_send, ag2_recv):
    cp, side = dims
    chips = cp // 2
    inner = 2 * side
    nreq, dmodel = x_v.shape
    nslab, latent, slab, nope = wuk_v.shape
    half_heads = nslab * slab
    heads = 2 * half_heads
    rope = kr_v.shape[1]
    half_rope = rope // 2
    tdev = cc_v.shape[1]
    wide = latent + LANES
    qk = nope + rope
    kdkv = wdkv_v.shape[1]
    own = heads // cp

    d = lax.axis_index('cp')
    c = lax.rem(d, 2)
    t = d // 2
    oc = 1 - c
    gi = lax.rem(d, inner)
    base = d - gi
    xx = gi // 2
    yy = d // inner
    partner = base + 2 * xx + oc

    kstep = 64

    def widen(src):
        def go(i, _):
            r = pl.multiple_of(i * kstep, kstep)
            stage_v[pl.ds(pl.multiple_of(r * slab, kstep * slab), kstep * slab), :] = (
                src[pl.ds(r, kstep)].astype(F32).reshape(kstep * slab, nope))
            return 0
        lax.fori_loop(0, latent // kstep, go, 0)

    def chip_at(r):
        return lax.rem(t + r, chips)

    pending = {}

    def done(name):
        pending.pop(name)()

    def drain():
        for name in list(pending):
            done(name)

    def local(name, src, dst, sem):
        cpy = pltpu.make_async_copy(src, dst, sem)
        cpy.start()
        pending[name] = cpy.wait

    later = []

    def issue(n):
        for _ in range(min(n, len(later))):
            for args in later.pop(0):
                local(*args)

    local('x', x_h, x_v, in_sem.at[0])
    nslot, krow, ucol = wuq_v.shape
    ndq = dmodel // krow
    for j in range(ndq):
        local(('dq', j), wdq_h.at[pl.ds(j * krow, krow), pl.ds(pl.multiple_of(c * ucol, LANES), ucol)], wuq_v.at[j], dq_sem.at[j])
    local('gq', gq_h, gq_v, in_sem.at[3])
    local('gkv', gkv_h, gkv_v, in_sem.at[4])
    local('freq', freq_h, freq_v, in_sem.at[5])
    nuq = wuq_h.shape[1] // 2 // ucol
    uslot = [(ndq + j) % nslot for j in range(nuq)]
    uks = [(('uk', s), wuk_h.at[:, pl.ds(pl.multiple_of(c * half_heads + s * slab, slab), slab), :], wuk_v.at[s], uk_sem.at[s])
           for s in range(nslab)]
    later.append([('dkv', wdkv_h.at[:, pl.ds(pl.multiple_of(gi * kdkv, LANES), kdkv)], wdkv_v, in_sem.at[2])] + uks[:nslab // 2])
    later.append(uks[nslab // 2:])
    for j in range(nuq):
        later.append([(('uq', j), wuq_h.at[:, pl.ds(pl.multiple_of(c * nuq * ucol + j * ucol, LANES), ucol)],
                       wuq_v.at[uslot[j]], uq_sem.at[j])])
    for b in range(nreq):
        later.append([(('cc', b), cc_h.at[b], cc_v.at[b], cc_sem.at[0, b]), (('kr', b), kr_h.at[b], kr_v.at[b], cc_sem.at[1, b])])
    head0 = c * half_heads + xx * slab + yy * own
    head_slab = head0 // slab
    head_in = head0 - head_slab * slab
    later.append([('uv', wuv_h.at[:, pl.ds(pl.multiple_of(head_slab * slab, slab), slab), :], wuv_v, in_sem.at[6])])
    later.append([('wo', wo_h.at[pl.ds(pl.multiple_of(head0 * nope, own * nope), own * nope), :], wo_v, in_sem.at[7])])

    barrier = pltpu.get_barrier_semaphore()

    def greet(r, _):
        pl.semaphore_signal(barrier, inc=1, device_id={'cp': 2 * chip_at(r) + c}, device_id_type=MESH)
        return 0

    lax.fori_loop(1, chips, greet, 0)
    for i in range(side):
        pl.semaphore_signal(barrier, inc=1, device_id={'cp': base + 2 * i + oc}, device_id_type=MESH)

    done('x')
    part = None
    for j in range(ndq):
        done(('dq', j))
        pj = dot(x_v[:, j * krow:(j + 1) * krow], wuq_v[j])
        part = pj if part is None else part + pj
        issue(1)
    cq_v[c] = part
    pl.semaphore_wait(barrier, chips - 1 + side)
    cq_copy = pltpu.make_async_remote_copy(src_ref=cq_v.at[c], dst_ref=cq_v.at[c], send_sem=a_send, recv_sem=a_recv,
                                           device_id={'cp': partner}, device_id_type=MESH)
    cq_copy.start()
    issue(2)
    pending['cq'] = cq_copy.wait

    def to_ring(buf, send, recv):
        def go(r, _):
            peer = lax.rem(gi + r, inner)
            pltpu.make_async_remote_copy(src_ref=buf.at[gi], dst_ref=buf.at[gi], send_sem=send, recv_sem=recv,
                                         device_id={'cp': base + peer}, device_id_type=MESH).start()
            return 0
        lax.fori_loop(1, inner, go, 0)

    done('dkv')
    kvp_v[gi, :, 0:latent + rope] = dot_nt(x_v[:, pl.ds(pl.multiple_of(gi * kdkv, LANES), kdkv)], wdkv_v[...])
    kvp_v[gi, :, latent + rope:] = jnp.zeros((nreq, wide - latent - rope), F32)
    to_ring(kvp_v, kv_send, kv_recv)
    pending['kv_send'] = lambda: wait_bytes(kvp_v.at[pl.ds(0, inner - 1)], kv_send)
    pending['kv_recv'] = lambda: wait_bytes(kvp_v.at[pl.ds(0, inner - 1)], kv_recv)

    xall = x_v[...].astype(F32)
    for i in range(2):
        xf_v[i] = xall[4 * i:4 * i + 4, :]
    rows = lax.broadcasted_iota(jnp.int32, (nreq, LANES), 0)
    ctx = jnp.zeros((nreq, LANES), jnp.int32)
    for b in range(nreq):
        ctx = jnp.where(rows == b, ctx_s[b], ctx)
    done('freq')
    angles = ctx.astype(F32) * freq_v[...]
    cos_full = jnp.cos(angles)[:, :rope]
    sin_raw = jnp.sin(angles)[:, :rope]
    lane = lax.broadcasted_iota(jnp.int32, (nreq, rope), 1)
    sin_full = jnp.where(lane < half_rope, -sin_raw, sin_raw)

    def rope_rotate(v):
        swapped = jnp.concatenate([v[:, half_rope:], v[:, :half_rope]], axis=1)
        return v * cos_full + swapped * sin_full

    for s in range(nslab):
        done(('uk', s))
        widen(wuk_v.at[s])
        issue(1)
        for i in range(slab):
            wk_v[s * slab + i] = stage_v[pl.ds(i, latent, stride=slab), :].astype(BF16)

    done('cq')
    cq = rounded(jnp.concatenate([cq_v[0], cq_v[1]], axis=1))
    done('gq')
    mean_sq = jnp.mean(cq * cq, axis=1, keepdims=True)
    cn = (cq * lax.rsqrt(mean_sq + NORM_EPS) * gq_v[...].reshape(1, gq_v.shape[0])).astype(BF16)
    row0 = c * half_heads * nreq
    zeros_pad = jnp.zeros((nreq, LANES - rope), F32)
    per = ucol // qk

    def q_slab_copy(s):
        view = q_v.at[:, pl.ds(pl.multiple_of(row0 + s * slab * nreq, slab * nreq), slab * nreq)]
        return pltpu.make_async_remote_copy(src_ref=view, dst_ref=view, send_sem=q_send.at[s], recv_sem=q_recv.at[s],
                                            device_id={'cp': partner}, device_id_type=MESH)

    def q_latent(j, qc):
        for i in range(per):
            h = j * per + i
            r = pl.multiple_of(row0 + h * nreq, nreq)
            qr = rounded(rope_rotate(qc[:, i * qk + nope:(i + 1) * qk]))
            q_v[latent // LANES, pl.ds(r, nreq), :] = jnp.concatenate([qr, zeros_pad], axis=1)
            ql = rounded(dot_nt(qc[:, i * qk:i * qk + nope].astype(BF16), wk_v[h]))
            for k in range(latent // LANES):
                q_v[k, pl.ds(r, nreq), :] = ql[:, k * LANES:(k + 1) * LANES]
        if (j + 1) * per % slab == 0:
            s = (j + 1) * per // slab - 1
            q_slab_copy(s).start()
            pending['q', s] = q_slab_copy(s).wait

    qc = None
    for j in range(nuq):
        done(('uq', j))
        issue(1)
        last, qc = qc, rounded(dot(cn, wuq_v[uslot[j]]))
        if j > 0:
            q_latent(j - 1, last)
    q_latent(nuq - 1, qc)
    issue(len(later))

    done('kv_recv')
    kv = kvp_v[0]
    for i in range(1, inner):
        kv = kv + kvp_v[i]
    kvl = kv[:, :latent]
    done('gkv')
    mean_sq = jnp.mean(kvl * kvl, axis=1, keepdims=True)
    c_new = kvl * lax.rsqrt(mean_sq + NORM_EPS) * gkv_v[...]
    kr_new = rope_rotate(kv[:, latent:latent + rope])
    out_v[:, dmodel:dmodel + latent] = c_new.astype(BF16)
    out_v[:, dmodel + latent:] = jnp.concatenate([kr_new, zeros_pad], axis=1).astype(BF16)
    cnf_v[:, :latent] = rounded(c_new)
    cnf_v[:, latent:] = jnp.concatenate([rounded(kr_new), zeros_pad], axis=1)

    for s in range(nslab):
        done(('q', s))

    scale = (nope + rope) ** -0.5
    block0 = d * tdev
    head_row = lax.broadcasted_iota(jnp.int32, (heads, 1), 0)
    mine0 = pl.multiple_of(c * half_heads, half_heads)
    theirs0 = pl.multiple_of(oc * half_heads, half_heads)

    def pair_copy(b):
        return pltpu.make_async_remote_copy(src_ref=acc_v.at[b, pl.ds(theirs0, half_heads)], dst_ref=pair_v.at[b],
                                            send_sem=pair_send.at[b], recv_sem=pair_recv.at[b],
                                            device_id={'cp': partner}, device_id_type=MESH)

    nkc = 4
    kc = tdev // nkc
    half_lane = lax.broadcasted_iota(jnp.int32, (heads, LANES), 1) < LANES // 2
    chunk_pos = lax.broadcasted_iota(jnp.int32, (heads, kc), 1)

    def q_of(b):
        return jnp.concatenate([q_v[k, pl.ds(b, heads, stride=nreq), :] for k in range(wide // LANES)], axis=1)

    def block_ready(b):
        done(('cc', b))
        done(('kr', b))

    def scores(b, s_ref):
        qb = q_of(b).astype(BF16)
        left = ctx_s[b] - block0
        m = None
        for k in range(nkc):
            cols = slice(k * kc, (k + 1) * kc)
            s = (dot_nt(qb[:, :latent], cc_v[b, cols]) + dot(qb[:, latent:latent + rope], kr_v[b, :, cols])) * scale
            s = jnp.where(chunk_pos < left - k * kc, s, MASKED)
            s_ref[:, cols] = s
            mk = jnp.max(s, axis=1, keepdims=True)
            m = mk if m is None else jnp.maximum(m, mk)
        m_v[b] = jnp.broadcast_to(m, (heads, LANES))

    def weigh(b, s_ref):
        qf = q_of(b)
        left = ctx_s[b] - block0
        new_row = cnf_v[b:b + 1, :]
        new_s = jnp.sum(qf * new_row, axis=1, keepdims=True) * scale
        at = head_row * 0 + left
        new_s = jnp.where(jnp.logical_and(at >= 0, at < tdev), new_s, MASKED)
        m = jnp.maximum(jnp.maximum(m_v[b][:, :1], new_s), FLOOR)
        new_w = jnp.exp(new_s - m)
        l = new_w
        acc = rounded(new_w) * new_row[:, :latent]
        for k in range(nkc):
            cols = slice(k * kc, (k + 1) * kc)
            p = jnp.exp(s_ref[:, cols] - m)
            l = l + jnp.sum(p, axis=1, keepdims=True)
            acc = acc + dot(p.astype(BF16), cc_v[b, cols])
        acc_v[b, :, :latent] = acc
        acc_v[b, :, latent:] = jnp.where(half_lane, m, l)

    quarter = half_heads // side

    def xs_copy(b, r):
        px = lax.rem(xx + r, side)
        return pltpu.make_async_remote_copy(src_ref=xs_v.at[b, pl.ds(pl.multiple_of(px * quarter, quarter), quarter)],
                                            dst_ref=xsr_v.at[b, r - 1], send_sem=xs_send.at[b], recv_sem=xs_recv.at[b],
                                            device_id={'cp': base + 2 * px + c}, device_id_type=MESH)

    def ys_copy(b, r):
        py = lax.rem(yy + r, side)
        return pltpu.make_async_remote_copy(src_ref=ys_v.at[b, py], dst_ref=ysr_v.at[b, r - 1],
                                            send_sem=ys_send.at[b], recv_sem=ys_recv.at[b],
                                            device_id={'cp': py * inner + gi}, device_id_type=MESH)

    def ml_of(v):
        return v[:, latent:latent + 1], v[:, wide - 1:wide]

    def merge(parts):
        ms, ls = zip(*[ml_of(p) for p in parts])
        m = functools.reduce(jnp.maximum, ms)
        fs = [jnp.exp(mi - m) for mi in ms]
        l = sum(f * li for f, li in zip(fs, ls))
        acc = sum(f * p[:, :latent] for f, p in zip(fs, parts))
        return m, l, acc

    def with_ml(m, l):
        side_lane = lax.broadcasted_iota(jnp.int32, (m.shape[0], LANES), 1)
        return jnp.where(side_lane < LANES // 2, m, l)

    def pair_merge(b):
        m, l, acc = merge([acc_v[b, pl.ds(mine0, half_heads), :], pair_v[b]])
        xs_v[b, :, :latent] = acc
        xs_v[b, :, latent:] = with_ml(m, l)

    def pair_sent(b):
        for r in range(1, side):
            xs_copy(b, r).start()

    def ring_merge(b):
        mine = xs_v[b, pl.ds(pl.multiple_of(xx * quarter, quarter), quarter), :]
        m, l, acc = merge([mine] + [xsr_v[b, r] for r in range(side - 1)])
        ml = with_ml(m, l)
        for k in range(side):
            ys_v[b, k, :, :latent] = acc[own * k:own * (k + 1), :]
            ys_v[b, k, :, latent:] = ml[own * k:own * (k + 1), :]

    def ring_sent(b):
        for r in range(1, side):
            ys_copy(b, r).start()

    lag = 5
    s_bufs = (sa_v, sb_v)
    block_ready(0)
    scores(0, s_bufs[0])
    for b in range(nreq):
        if b + 1 < nreq:
            block_ready(b + 1)
        if b > 0:
            pair_copy(b - 1).wait_recv()
        if b >= lag:
            wait_bytes(xsr_v.at[b - lag], xs_recv.at[b - lag])
        if b + 1 < nreq:
            scores(b + 1, s_bufs[(b + 1) % 2])
        weigh(b, s_bufs[b % 2])
        if b > 0:
            pair_merge(b - 1)
        if b >= lag:
            ring_merge(b - lag)
        pair_copy(b).start()
        pending['pair', b] = pair_copy(b).wait_send
        if b > 0:
            pair_sent(b - 1)
        if b >= lag:
            ring_sent(b - lag)
    pair_copy(nreq - 1).wait_recv()
    pair_merge(nreq - 1)
    pair_sent(nreq - 1)
    for b in range(nreq - lag, nreq):
        wait_bytes(xsr_v.at[b], xs_recv.at[b])
        ring_merge(b)
        ring_sent(b)

    def each(view, sem):
        def go(b, _):
            wait_bytes(view.at[b], sem.at[b])
            return 0
        return lambda: lax.fori_loop(0, nreq, go, 0)

    pending['xs_send'] = each(xsr_v, xs_send)
    pending['ys_send'] = each(ysr_v, ys_send)
    pending['ys_recv'] = each(ysr_v, ys_recv)

    done('uv')
    widen(wuv_v)
    for k in range(own):
        wv_v[k] = stage_v[pl.ds(head_in + k, latent, stride=slab), :].astype(BF16)

    def owner_merge(b, _):
        wait_bytes(ysr_v.at[b], ys_recv.at[b])
        m, l, acc = merge([ys_v[b, yy]] + [ysr_v[b, r] for r in range(side - 1)])
        ol = rounded(acc / l)
        for k in range(own):
            olat_v[k, pl.ds(b, 1), :] = ol[k:k + 1, :]
        return 0

    lax.fori_loop(0, nreq, owner_merge, 0)
    pending.pop('ys_recv')

    done('wo')
    outs = []
    for k in range(own):
        outs.append(dot(olat_v[k].astype(BF16), wv_v[k]).astype(BF16))
    o = jnp.concatenate(outs, axis=1)
    ncol = 768
    for j in range(dmodel // ncol):
        pj = dot(o, wo_v[:, j * ncol:(j + 1) * ncol])
        for i in range(2):
            po_v[i, :, j * ncol:(j + 1) * ncol] = pj[4 * i:4 * i + 4, :]
    po_copy = pltpu.make_async_remote_copy(src_ref=po_v.at[oc], dst_ref=pop_v, send_sem=po_send, recv_sem=po_recv,
                                           device_id={'cp': partner}, device_id_type=MESH)
    po_copy.start()
    po_copy.wait()
    tcol = dmodel // chips
    for k in range(chips):
        pt_v[k] = po_v[c, :, k * tcol:(k + 1) * tcol] + pop_v[:, k * tcol:(k + 1) * tcol]

    def pt_go(r, _):
        pltpu.make_async_remote_copy(src_ref=pt_v.at[chip_at(r)], dst_ref=ptr_v.at[r - 1], send_sem=pt_send, recv_sem=pt_recv,
                                     device_id={'cp': 2 * chip_at(r) + c}, device_id_type=MESH).start()
        return 0
    lax.fori_loop(1, chips, pt_go, 0)
    pending['pt_send'] = lambda: wait_bytes(ptr_v, pt_send)
    wait_bytes(ptr_v, pt_recv)
    tot = pt_v[t]
    for r in range(chips - 1):
        tot = tot + ptr_v[r]
    ag_v[c, t] = rounded(xf_v[c, :, pl.ds(pl.multiple_of(t * tcol, LANES), tcol)] + tot)

    def ag_go(r, _):
        pltpu.make_async_remote_copy(src_ref=ag_v.at[c, t], dst_ref=ag_v.at[c, t], send_sem=ag_send, recv_sem=ag_recv,
                                     device_id={'cp': 2 * chip_at(r) + c}, device_id_type=MESH).start()
        return 0
    lax.fori_loop(1, chips, ag_go, 0)
    pending['ag_send'] = lambda: wait_bytes(ag_v.at[0, pl.ds(0, chips - 1)], ag_send)
    wait_bytes(ag_v.at[0, pl.ds(0, chips - 1)], ag_recv)
    ag_copy = pltpu.make_async_remote_copy(src_ref=ag_v.at[c], dst_ref=ag_v.at[c], send_sem=ag2_send, recv_sem=ag2_recv,
                                           device_id={'cp': partner}, device_id_type=MESH)
    ag_copy.start()
    ag_copy.wait()
    for k in range(chips):
        out_v[:, k * tcol:(k + 1) * tcol] = jnp.concatenate([ag_v[0, k], ag_v[1, k]], axis=0).astype(BF16)

    drain()


def split_outputs(packed_v, xo_v, cn_v, kr_v):
    dmodel, latent, rope = xo_v.shape[1], cn_v.shape[1], kr_v.shape[1]
    xo_v[...] = packed_v[:, :dmodel]
    cn_v[...] = packed_v[:, dmodel:dmodel + latent]
    kr_v[...] = packed_v[:, dmodel + latent:dmodel + latent + rope]


def solution(mesh):
    cp = mesh.shape['cp']
    side = math.isqrt(cp // 2)
    inner = 2 * side
    chips = cp // 2

    def decode_step(x, w_dq, g_q, w_uq, w_dkv, g_kv, w_uk, w_uv, w_o, cache_c, cache_kr, ctx_len):
        nreq, dmodel = x.shape
        qlora = w_dq.shape[1]
        latent, heads, nope = w_uk.shape
        rope = cache_kr.shape[2]
        tdev = cache_c.shape[1]
        half = heads // 2
        own = heads // cp
        wide = latent + LANES
        tcol = dmodel // chips
        inv = (np.float64(ROPE_THETA) ** (-2.0 * np.arange(rope // 2) / rope)).astype(np.float32)
        freq = np.zeros((1, LANES), np.float32)
        freq[0, :rope] = np.concatenate([inv, inv])
        anyspec = pl.BlockSpec(memory_space=pl.ANY)
        dma = pltpu.SemaphoreType.DMA
        vm = pltpu.VMEM
        out_shape = (jax.ShapeDtypeStruct((nreq, dmodel), BF16), jax.ShapeDtypeStruct((nreq, latent), BF16),
                     jax.ShapeDtypeStruct((nreq, rope), BF16))
        scratch = [
            vm((nreq, dmodel), BF16), vm((qlora,), F32),
            vm((w_uq.shape[1] // qlora, qlora, qlora // 2), BF16), vm((w_dkv.shape[1], dmodel // inner), BF16), vm((1, latent), F32),
            vm((half // 8, latent, 8, nope), BF16), vm((latent, 8, nope), BF16), vm((own * nope, dmodel), BF16),
            vm((nreq, tdev, latent), BF16), vm((nreq, rope, tdev), BF16), vm((1, LANES), F32), vm((own, latent, nope), BF16),
            vm((half, latent, nope), BF16), vm((latent * 8, nope), F32),
            vm((2, nreq // 2, dmodel), F32), vm((2, nreq, qlora // 2), F32), vm((inner, nreq, wide), F32),
            vm((wide // LANES, heads * nreq, LANES), F32), vm((nreq, wide), F32),
            vm((heads, tdev), F32), vm((heads, tdev), F32), vm((nreq, heads, LANES), F32),
            vm((nreq, heads, wide), F32), vm((nreq, half, wide), F32),
            vm((nreq, half, wide), F32), vm((nreq, side - 1, half // side, wide), F32),
            vm((nreq, side, own, wide), F32), vm((nreq, side - 1, own, wide), F32), vm((own, nreq, latent), F32),
            vm((2, nreq // 2, dmodel), F32), vm((nreq // 2, dmodel), F32),
            vm((chips, nreq // 2, tcol), F32), vm((chips - 1, nreq // 2, tcol), F32), vm((2, chips, nreq // 2, tcol), F32),
            dma((8,)), dma((dmodel // qlora,)), dma((w_uq.shape[1] // qlora,)), dma((half // 8,)), dma((2, nreq)),
            dma, dma, dma, dma, dma((half // 8,)), dma((half // 8,)), dma((nreq,)), dma((nreq,)), dma((nreq,)), dma((nreq,)), dma((nreq,)), dma((nreq,)),
            dma, dma, dma, dma, dma, dma, dma, dma,
        ]
        packed = pl.pallas_call(
            functools.partial(step_kernel, (cp, side)),
            out_shape=jax.ShapeDtypeStruct((nreq, dmodel + wide), BF16),
            in_specs=[anyspec] * 12 + [pl.BlockSpec(memory_space=pltpu.SMEM)],
            out_specs=pl.BlockSpec(memory_space=pltpu.VMEM),
            scratch_shapes=scratch,
            compiler_params=pltpu.CompilerParams(collective_id=0, has_side_effects=True, vmem_limit_bytes=67043328),
            name='decode_step',
        )(x, w_dq, g_q, w_uq, w_dkv.T, g_kv.reshape(1, latent), w_uk, w_uv, w_o,
          cache_c, jnp.swapaxes(cache_kr, 1, 2), jnp.asarray(freq), ctx_len)
        vspec = pl.BlockSpec(memory_space=pltpu.VMEM)
        return pl.pallas_call(split_outputs, out_shape=out_shape, in_specs=[vspec], out_specs=(vspec,) * 3,
                              name='split_outputs')(packed)

    spec_rows = P('dp', None)
    spec_cache = P('dp', 'cp', None)
    in_specs = (spec_rows, P(), P(), P(), P(), P(), P(), P(), P(), spec_cache, spec_cache, P('dp'))
    out_specs = (spec_rows, spec_rows, spec_rows)
    return jax.shard_map(decode_step, mesh=mesh, in_specs=in_specs, out_specs=out_specs, check_vma=False)
```

```python
import functools
import math

import jax
import jax.numpy as jnp
import numpy as np
from jax import lax
from jax.experimental import pallas as pl
from jax.experimental.pallas import tpu as pltpu
from jax.sharding import PartitionSpec as P

NORM_EPS = 1e-6
ROPE_THETA = 10000.0
MASKED = -1e30
FLOOR = -1e29
F32, BF16 = jnp.float32, jnp.bfloat16
MESH = pl.DeviceIdType.MESH
NT = (((1,), (1,)), ((), ()))
LANES = 128


def dot(a, b):
    return jnp.dot(a, b, preferred_element_type=F32)


def dot_nt(a, b):
    return lax.dot_general(a, b, NT, preferred_element_type=F32)


def rounded(v):
    return v.astype(BF16).astype(F32)


def wait_bytes(view, sem):
    pltpu.make_async_copy(view, view, sem).wait()


def step_kernel(dims, x_h, wdq_h, gq_h, wuq_h, wdkv_h, gkv_h, wuk_h, wuv_h, wo_h, cc_h, kr_h, freq_h, ctx_s,
                out_v,
                x_v, gq_v, wuq_v, wdkv_v, gkv_v, wuk_v, wuv_v, wo_v, cc_v, kr_v, freq_v, wv_v, wk_v, stage_v,
                xf_v, cq_v, kvp_v, q_v, cnf_v, sa_v, sb_v, m_v, acc_v, pair_v, xs_v, xsr_v, ys_v, ysr_v, olat_v, po_v, pop_v, pt_v, ptr_v, ag_v,
                in_sem, dq_sem, uq_sem, uk_sem, cc_sem,
                a_send, a_recv, kv_send, kv_recv, q_send, q_recv, pair_send, pair_recv, xs_send, xs_recv, ys_send, ys_recv,
                po_send, po_recv, pt_send, pt_recv, ag_send, ag_recv, ag2_send, ag2_recv):
    cp, side = dims
    chips = cp // 2
    inner = 2 * side
    nreq, dmodel = x_v.shape
    nslab, latent, slab, nope = wuk_v.shape
    half_heads = nslab * slab
    heads = 2 * half_heads
    rope = kr_v.shape[1]
    half_rope = rope // 2
    tdev = cc_v.shape[1]
    wide = latent + LANES
    qk = nope + rope
    kdkv = wdkv_v.shape[1]
    own = heads // cp

    d = lax.axis_index('cp')
    c = lax.rem(d, 2)
    t = d // 2
    oc = 1 - c
    gi = lax.rem(d, inner)
    base = d - gi
    xx = gi // 2
    yy = d // inner
    partner = base + 2 * xx + oc

    kstep = 64

    def widen(src):
        def go(i, _):
            r = pl.multiple_of(i * kstep, kstep)
            stage_v[pl.ds(pl.multiple_of(r * slab, kstep * slab), kstep * slab), :] = (
                src[pl.ds(r, kstep)].astype(F32).reshape(kstep * slab, nope))
            return 0
        lax.fori_loop(0, latent // kstep, go, 0)

    def chip_at(r):
        return lax.rem(t + r, chips)

    pending = {}

    def done(name):
        pending.pop(name)()

    def drain():
        for name in list(pending):
            done(name)

    def local(name, src, dst, sem):
        cpy = pltpu.make_async_copy(src, dst, sem)
        cpy.start()
        pending[name] = cpy.wait

    local('x', x_h, x_v, in_sem.at[0])
    nslot, krow, ucol = wuq_v.shape
    ndq = dmodel // krow
    for j in range(ndq):
        pltpu.make_async_copy(wdq_h.at[pl.ds(j * krow, krow), pl.ds(pl.multiple_of(c * ucol, LANES), ucol)],
                              wuq_v.at[j], dq_sem.at[j]).start()
    local('gq', gq_h, gq_v, in_sem.at[3])
    local('gkv', gkv_h, gkv_v, in_sem.at[4])
    local('freq', freq_h, freq_v, in_sem.at[5])
    nuq = wuq_h.shape[1] // 2 // ucol

    def uq_copy(j):
        return pltpu.make_async_copy(wuq_h.at[:, pl.ds(pl.multiple_of((c * nuq + j) * ucol, LANES), ucol)],
                                     wuq_v.at[lax.rem(ndq + j, nslot)], uq_sem.at[j])

    def uk_copy(s):
        return pltpu.make_async_copy(wuk_h.at[:, pl.ds(pl.multiple_of(c * half_heads + s * slab, slab), slab), :],
                                     wuk_v.at[s], uk_sem.at[s])

    def cache_copies(b):
        return (pltpu.make_async_copy(cc_h.at[b], cc_v.at[b], cc_sem.at[0, b]),
                pltpu.make_async_copy(kr_h.at[b], kr_v.at[b], cc_sem.at[1, b]))

    def cache_start(b):
        for cpy in cache_copies(b):
            cpy.start()

    def cache_wait(b):
        for cpy in cache_copies(b):
            cpy.wait()

    head0 = c * half_heads + xx * slab + yy * own
    head_slab = head0 // slab
    head_in = head0 - head_slab * slab

    barrier = pltpu.get_barrier_semaphore()

    def greet(r, _):
        pl.semaphore_signal(barrier, inc=1, device_id={'cp': 2 * chip_at(r) + c}, device_id_type=MESH)
        return 0

    lax.fori_loop(1, chips, greet, 0)
    for i in range(side):
        pl.semaphore_signal(barrier, inc=1, device_id={'cp': base + 2 * i + oc}, device_id_type=MESH)

    done('x')
    local('dkv', wdkv_h.at[:, pl.ds(pl.multiple_of(gi * kdkv, LANES), kdkv)], wdkv_v, in_sem.at[2])
    for s in range(nslab):
        uk_copy(s).start()

    def a_step(j, part):
        pltpu.make_async_copy(wuq_v.at[j], wuq_v.at[j], dq_sem.at[j]).wait()

        @pl.when(j >= 2)
        def _():
            uq_copy(j - 2).start()
        return part + dot(x_v[:, pl.ds(pl.multiple_of(j * krow, krow), krow)], wuq_v[j])

    part = lax.fori_loop(0, ndq, a_step, jnp.zeros((nreq, ucol), F32))
    cq_v[c] = part
    pl.semaphore_wait(barrier, chips - 1 + side)
    cq_copy = pltpu.make_async_remote_copy(src_ref=cq_v.at[c], dst_ref=cq_v.at[c], send_sem=a_send, recv_sem=a_recv,
                                           device_id={'cp': partner}, device_id_type=MESH)
    cq_copy.start()
    for j in range(ndq - 2, nslot - ndq):
        uq_copy(j).start()
    pending['cq'] = cq_copy.wait

    def to_ring(buf, send, recv):
        def go(r, _):
            peer = lax.rem(gi + r, inner)
            pltpu.make_async_remote_copy(src_ref=buf.at[gi], dst_ref=buf.at[gi], send_sem=send, recv_sem=recv,
                                         device_id={'cp': base + peer}, device_id_type=MESH).start()
            return 0
        lax.fori_loop(1, inner, go, 0)

    done('dkv')
    kvp_v[gi, :, 0:latent + rope] = dot_nt(x_v[:, pl.ds(pl.multiple_of(gi * kdkv, LANES), kdkv)], wdkv_v[...])
    kvp_v[gi, :, latent + rope:] = jnp.zeros((nreq, wide - latent - rope), F32)
    to_ring(kvp_v, kv_send, kv_recv)
    pending['kv_send'] = lambda: wait_bytes(kvp_v.at[pl.ds(0, inner - 1)], kv_send)
    pending['kv_recv'] = lambda: wait_bytes(kvp_v.at[pl.ds(0, inner - 1)], kv_recv)

    xall = x_v[...].astype(F32)
    for i in range(2):
        xf_v[i] = xall[4 * i:4 * i + 4, :]
    rows = lax.broadcasted_iota(jnp.int32, (nreq, LANES), 0)
    ctx = jnp.zeros((nreq, LANES), jnp.int32)
    for b in range(nreq):
        ctx = jnp.where(rows == b, ctx_s[b], ctx)
    done('freq')
    angles = ctx.astype(F32) * freq_v[...]
    cos_full = jnp.cos(angles)[:, :rope]
    sin_raw = jnp.sin(angles)[:, :rope]
    lane = lax.broadcasted_iota(jnp.int32, (nreq, rope), 1)
    sin_full = jnp.where(lane < half_rope, -sin_raw, sin_raw)

    def rope_rotate(v):
        swapped = jnp.concatenate([v[:, half_rope:], v[:, :half_rope]], axis=1)
        return v * cos_full + swapped * sin_full

    def uk_step(s, _):
        uk_copy(s).wait()
        uq_copy(nslot - ndq + s).start()
        widen(wuk_v.at[s])

        def head_step(i, _):
            wk_v[s * slab + i] = stage_v[pl.ds(i, latent, stride=slab), :].astype(BF16)
            return 0
        lax.fori_loop(0, slab, head_step, 0)
        return 0

    lax.fori_loop(0, nslab, uk_step, 0)

    done('cq')
    cq = rounded(jnp.concatenate([cq_v[0], cq_v[1]], axis=1))
    done('gq')
    mean_sq = jnp.mean(cq * cq, axis=1, keepdims=True)
    cn = (cq * lax.rsqrt(mean_sq + NORM_EPS) * gq_v[...].reshape(1, gq_v.shape[0])).astype(BF16)
    row0 = c * half_heads * nreq
    zeros_pad = jnp.zeros((nreq, LANES - rope), F32)
    per = ucol // qk

    def q_slab_copy(s):
        view = q_v.at[:, pl.ds(pl.multiple_of(row0 + s * slab * nreq, slab * nreq), slab * nreq)]
        return pltpu.make_async_remote_copy(src_ref=view, dst_ref=view, send_sem=q_send.at[s], recv_sem=q_recv.at[s],
                                            device_id={'cp': partner}, device_id_type=MESH)

    def q_latent(j, qc):
        for i in range(per):
            h = j * per + i
            r = pl.multiple_of(row0 + h * nreq, nreq)
            qr = rounded(rope_rotate(qc[:, i * qk + nope:(i + 1) * qk]))
            q_v[latent // LANES, pl.ds(r, nreq), :] = jnp.concatenate([qr, zeros_pad], axis=1)
            ql = rounded(dot_nt(qc[:, i * qk:i * qk + nope].astype(BF16), wk_v[h]))
            for k in range(latent // LANES):
                q_v[k, pl.ds(r, nreq), :] = ql[:, k * LANES:(k + 1) * LANES]
    def b_step(j, last):
        uq_copy(j).wait()
        cache_start(j - 1)
        qc = rounded(dot(cn, wuq_v[lax.rem(ndq + j, nslot)]))
        q_latent(j - 1, last)

        @pl.when(lax.rem(j * per, slab) == 0)
        def _():
            q_slab_copy(j * per // slab - 1).start()
        return qc

    uq_copy(0).wait()
    qc = lax.fori_loop(1, nuq, b_step, rounded(dot(cn, wuq_v[ndq])))
    cache_start(nuq - 1)
    q_latent(nuq - 1, qc)
    q_slab_copy(nslab - 1).start()
    for s in range(nslab):
        pending['q', s] = q_slab_copy(s).wait
    local('uv', wuv_h.at[:, pl.ds(pl.multiple_of(head_slab * slab, slab), slab), :], wuv_v, in_sem.at[6])
    local('wo', wo_h.at[pl.ds(pl.multiple_of(head0 * nope, own * nope), own * nope), :], wo_v, in_sem.at[7])

    done('kv_recv')
    kv = kvp_v[0]
    for i in range(1, inner):
        kv = kv + kvp_v[i]
    kvl = kv[:, :latent]
    done('gkv')
    mean_sq = jnp.mean(kvl * kvl, axis=1, keepdims=True)
    c_new = kvl * lax.rsqrt(mean_sq + NORM_EPS) * gkv_v[...]
    kr_new = rope_rotate(kv[:, latent:latent + rope])
    out_v[:, dmodel:dmodel + latent] = c_new.astype(BF16)
    out_v[:, dmodel + latent:] = jnp.concatenate([kr_new, zeros_pad], axis=1).astype(BF16)
    cnf_v[:, :latent] = rounded(c_new)
    cnf_v[:, latent:] = jnp.concatenate([rounded(kr_new), zeros_pad], axis=1)

    for s in range(nslab):
        done(('q', s))

    scale = (nope + rope) ** -0.5
    block0 = d * tdev
    head_row = lax.broadcasted_iota(jnp.int32, (heads, 1), 0)
    mine0 = pl.multiple_of(c * half_heads, half_heads)
    theirs0 = pl.multiple_of(oc * half_heads, half_heads)

    def pair_copy(b):
        return pltpu.make_async_remote_copy(src_ref=acc_v.at[b, pl.ds(theirs0, half_heads)], dst_ref=pair_v.at[b],
                                            send_sem=pair_send.at[b], recv_sem=pair_recv.at[b],
                                            device_id={'cp': partner}, device_id_type=MESH)

    nkc = 4
    kc = tdev // nkc
    half_lane = lax.broadcasted_iota(jnp.int32, (heads, LANES), 1) < LANES // 2
    chunk_pos = lax.broadcasted_iota(jnp.int32, (heads, kc), 1)

    def q_of(b):
        return jnp.concatenate([q_v[k, pl.ds(b, heads, stride=nreq), :] for k in range(wide // LANES)], axis=1)

    def scores(b, s_ref):
        qb = q_of(b).astype(BF16)
        left = ctx_s[b] - block0
        m = None
        for k in range(nkc):
            cols = slice(k * kc, (k + 1) * kc)
            s = (dot_nt(qb[:, :latent], cc_v[b, cols]) + dot(qb[:, latent:latent + rope], kr_v[b, :, cols])) * scale
            s = jnp.where(chunk_pos < left - k * kc, s, MASKED)
            s_ref[:, cols] = s
            mk = jnp.max(s, axis=1, keepdims=True)
            m = mk if m is None else jnp.maximum(m, mk)
        m_v[b] = jnp.broadcast_to(m, (heads, LANES))

    def weigh(b, s_ref):
        qf = q_of(b)
        left = ctx_s[b] - block0
        new_row = cnf_v[pl.ds(b, 1), :]
        new_s = jnp.sum(qf * new_row, axis=1, keepdims=True) * scale
        at = head_row * 0 + left
        new_s = jnp.where(jnp.logical_and(at >= 0, at < tdev), new_s, MASKED)
        m = jnp.maximum(jnp.maximum(m_v[b][:, :1], new_s), FLOOR)
        new_w = jnp.exp(new_s - m)
        l = new_w
        acc = rounded(new_w) * new_row[:, :latent]
        for k in range(nkc):
            cols = slice(k * kc, (k + 1) * kc)
            p = jnp.exp(s_ref[:, cols] - m)
            l = l + jnp.sum(p, axis=1, keepdims=True)
            acc = acc + dot(p.astype(BF16), cc_v[b, cols])
        acc_v[b, :, :latent] = acc
        acc_v[b, :, latent:] = jnp.where(half_lane, m, l)

    quarter = half_heads // side

    def xs_copy(b, r):
        px = lax.rem(xx + r, side)
        return pltpu.make_async_remote_copy(src_ref=xs_v.at[b, pl.ds(pl.multiple_of(px * quarter, quarter), quarter)],
                                            dst_ref=xsr_v.at[b, r - 1], send_sem=xs_send.at[b], recv_sem=xs_recv.at[b],
                                            device_id={'cp': base + 2 * px + c}, device_id_type=MESH)

    def ys_copy(b, r):
        py = lax.rem(yy + r, side)
        return pltpu.make_async_remote_copy(src_ref=ys_v.at[b, py], dst_ref=ysr_v.at[b, r - 1],
                                            send_sem=ys_send.at[b], recv_sem=ys_recv.at[b],
                                            device_id={'cp': py * inner + gi}, device_id_type=MESH)

    def ml_of(v):
        return v[:, latent:latent + 1], v[:, wide - 1:wide]

    def merge(parts):
        ms, ls = zip(*[ml_of(p) for p in parts])
        m = functools.reduce(jnp.maximum, ms)
        fs = [jnp.exp(mi - m) for mi in ms]
        l = sum(f * li for f, li in zip(fs, ls))
        acc = sum(f * p[:, :latent] for f, p in zip(fs, parts))
        return m, l, acc

    def with_ml(m, l):
        side_lane = lax.broadcasted_iota(jnp.int32, (m.shape[0], LANES), 1)
        return jnp.where(side_lane < LANES // 2, m, l)

    def pair_merge(b):
        m, l, acc = merge([acc_v[b, pl.ds(mine0, half_heads), :], pair_v[b]])
        xs_v[b, :, :latent] = acc
        xs_v[b, :, latent:] = with_ml(m, l)

    def pair_sent(b):
        for r in range(1, side):
            xs_copy(b, r).start()

    def ring_merge(b):
        mine = xs_v[b, pl.ds(pl.multiple_of(xx * quarter, quarter), quarter), :]
        m, l, acc = merge([mine] + [xsr_v[b, r] for r in range(side - 1)])
        ml = with_ml(m, l)
        for k in range(side):
            ys_v[b, k, :, :latent] = acc[own * k:own * (k + 1), :]
            ys_v[b, k, :, latent:] = ml[own * k:own * (k + 1), :]

    def ring_sent(b):
        for r in range(1, side):
            ys_copy(b, r).start()

    def pair_step(b):
        pair_copy(b).wait_recv()
        pair_merge(b)
        pair_sent(b)

    def two_requests(i, _):
        b = 2 * i
        cache_wait(b + 1)
        scores(b + 1, sb_v)
        weigh(b, sa_v)
        pair_copy(b).start()

        @pl.when(i > 0)
        def _():
            pair_step(b - 1)

        @pl.when(b + 2 < nreq)
        def _():
            cache_wait(b + 2)
        scores(jnp.minimum(b + 2, nreq - 1), sa_v)
        weigh(b + 1, sb_v)
        pair_copy(b + 1).start()
        pair_step(b)
        return 0

    cache_wait(0)
    scores(0, sa_v)
    lax.fori_loop(0, nreq // 2, two_requests, 0)
    for b in range(nreq):
        pending['pair', b] = pair_copy(b).wait_send

    def ring_step(b, _):
        wait_bytes(xsr_v.at[b], xs_recv.at[b])
        ring_merge(b)
        ring_sent(b)
        return 0

    lax.fori_loop(0, 2, ring_step, 0)
    pair_step(nreq - 1)
    lax.fori_loop(2, nreq, ring_step, 0)

    def each(view, sem):
        def go(b, _):
            wait_bytes(view.at[b], sem.at[b])
            return 0
        return lambda: lax.fori_loop(0, nreq, go, 0)

    pending['xs_send'] = each(xsr_v, xs_send)
    pending['ys_send'] = each(ysr_v, ys_send)
    pending['ys_recv'] = each(ysr_v, ys_recv)

    done('uv')
    widen(wuv_v)
    for k in range(own):
        wv_v[k] = stage_v[pl.ds(head_in + k, latent, stride=slab), :].astype(BF16)

    def owner_merge(b, _):
        wait_bytes(ysr_v.at[b], ys_recv.at[b])
        m, l, acc = merge([ys_v[b, yy]] + [ysr_v[b, r] for r in range(side - 1)])
        ol = rounded(acc / l)
        for k in range(own):
            olat_v[k, pl.ds(b, 1), :] = ol[k:k + 1, :]
        return 0

    lax.fori_loop(0, nreq, owner_merge, 0)
    pending.pop('ys_recv')

    done('wo')
    outs = []
    for k in range(own):
        outs.append(dot(olat_v[k].astype(BF16), wv_v[k]).astype(BF16))
    o = jnp.concatenate(outs, axis=1)
    ncol = 768
    for j in range(dmodel // ncol):
        pj = dot(o, wo_v[:, j * ncol:(j + 1) * ncol])
        for i in range(2):
            po_v[i, :, j * ncol:(j + 1) * ncol] = pj[4 * i:4 * i + 4, :]
    po_copy = pltpu.make_async_remote_copy(src_ref=po_v.at[oc], dst_ref=pop_v, send_sem=po_send, recv_sem=po_recv,
                                           device_id={'cp': partner}, device_id_type=MESH)
    po_copy.start()
    po_copy.wait()
    tcol = dmodel // chips
    for k in range(chips):
        pt_v[k] = po_v[c, :, k * tcol:(k + 1) * tcol] + pop_v[:, k * tcol:(k + 1) * tcol]

    def pt_go(r, _):
        pltpu.make_async_remote_copy(src_ref=pt_v.at[chip_at(r)], dst_ref=ptr_v.at[r - 1], send_sem=pt_send, recv_sem=pt_recv,
                                     device_id={'cp': 2 * chip_at(r) + c}, device_id_type=MESH).start()
        return 0
    lax.fori_loop(1, chips, pt_go, 0)
    pending['pt_send'] = lambda: wait_bytes(ptr_v, pt_send)
    wait_bytes(ptr_v, pt_recv)
    tot = pt_v[t]
    for r in range(chips - 1):
        tot = tot + ptr_v[r]
    ag_v[c, t] = rounded(xf_v[c, :, pl.ds(pl.multiple_of(t * tcol, LANES), tcol)] + tot)

    def ag_go(r, _):
        pltpu.make_async_remote_copy(src_ref=ag_v.at[c, t], dst_ref=ag_v.at[c, t], send_sem=ag_send, recv_sem=ag_recv,
                                     device_id={'cp': 2 * chip_at(r) + c}, device_id_type=MESH).start()
        return 0
    lax.fori_loop(1, chips, ag_go, 0)
    pending['ag_send'] = lambda: wait_bytes(ag_v.at[0, pl.ds(0, chips - 1)], ag_send)
    wait_bytes(ag_v.at[0, pl.ds(0, chips - 1)], ag_recv)
    ag_copy = pltpu.make_async_remote_copy(src_ref=ag_v.at[c], dst_ref=ag_v.at[c], send_sem=ag2_send, recv_sem=ag2_recv,
                                           device_id={'cp': partner}, device_id_type=MESH)
    ag_copy.start()
    ag_copy.wait()
    for k in range(chips):
        out_v[:, k * tcol:(k + 1) * tcol] = jnp.concatenate([ag_v[0, k], ag_v[1, k]], axis=0).astype(BF16)

    drain()


def split_outputs(packed_v, xo_v, cn_v, kr_v):
    dmodel, latent, rope = xo_v.shape[1], cn_v.shape[1], kr_v.shape[1]
    xo_v[...] = packed_v[:, :dmodel]
    cn_v[...] = packed_v[:, dmodel:dmodel + latent]
    kr_v[...] = packed_v[:, dmodel + latent:dmodel + latent + rope]


def solution(mesh):
    cp = mesh.shape['cp']
    side = math.isqrt(cp // 2)
    inner = 2 * side
    chips = cp // 2

    def decode_step(x, w_dq, g_q, w_uq, w_dkv, g_kv, w_uk, w_uv, w_o, cache_c, cache_kr, ctx_len):
        nreq, dmodel = x.shape
        qlora = w_dq.shape[1]
        latent, heads, nope = w_uk.shape
        rope = cache_kr.shape[2]
        tdev = cache_c.shape[1]
        half = heads // 2
        own = heads // cp
        wide = latent + LANES
        tcol = dmodel // chips
        inv = (np.float64(ROPE_THETA) ** (-2.0 * np.arange(rope // 2) / rope)).astype(np.float32)
        freq = np.zeros((1, LANES), np.float32)
        freq[0, :rope] = np.concatenate([inv, inv])
        anyspec = pl.BlockSpec(memory_space=pl.ANY)
        dma = pltpu.SemaphoreType.DMA
        vm = pltpu.VMEM
        out_shape = (jax.ShapeDtypeStruct((nreq, dmodel), BF16), jax.ShapeDtypeStruct((nreq, latent), BF16),
                     jax.ShapeDtypeStruct((nreq, rope), BF16))
        scratch = [
            vm((nreq, dmodel), BF16), vm((qlora,), F32),
            vm((w_uq.shape[1] // qlora, qlora, qlora // 2), BF16), vm((w_dkv.shape[1], dmodel // inner), BF16), vm((1, latent), F32),
            vm((half // 8, latent, 8, nope), BF16), vm((latent, 8, nope), BF16), vm((own * nope, dmodel), BF16),
            vm((nreq, tdev, latent), BF16), vm((nreq, rope, tdev), BF16), vm((1, LANES), F32), vm((own, latent, nope), BF16),
            vm((half, latent, nope), BF16), vm((latent * 8, nope), F32),
            vm((2, nreq // 2, dmodel), F32), vm((2, nreq, qlora // 2), F32), vm((inner, nreq, wide), F32),
            vm((wide // LANES, heads * nreq, LANES), F32), vm((nreq, wide), F32),
            vm((heads, tdev), F32), vm((heads, tdev), F32), vm((nreq, heads, LANES), F32),
            vm((nreq, heads, wide), F32), vm((nreq, half, wide), F32),
            vm((nreq, half, wide), F32), vm((nreq, side - 1, half // side, wide), F32),
            vm((nreq, side, own, wide), F32), vm((nreq, side - 1, own, wide), F32), vm((own, nreq, latent), F32),
            vm((2, nreq // 2, dmodel), F32), vm((nreq // 2, dmodel), F32),
            vm((chips, nreq // 2, tcol), F32), vm((chips - 1, nreq // 2, tcol), F32), vm((2, chips, nreq // 2, tcol), F32),
            dma((8,)), dma((dmodel // qlora,)), dma((w_uq.shape[1] // qlora,)), dma((half // 8,)), dma((2, nreq)),
            dma, dma, dma, dma, dma((half // 8,)), dma((half // 8,)), dma((nreq,)), dma((nreq,)), dma((nreq,)), dma((nreq,)), dma((nreq,)), dma((nreq,)),
            dma, dma, dma, dma, dma, dma, dma, dma,
        ]
        packed = pl.pallas_call(
            functools.partial(step_kernel, (cp, side)),
            out_shape=jax.ShapeDtypeStruct((nreq, dmodel + wide), BF16),
            in_specs=[anyspec] * 12 + [pl.BlockSpec(memory_space=pltpu.SMEM)],
            out_specs=pl.BlockSpec(memory_space=pltpu.VMEM),
            scratch_shapes=scratch,
            compiler_params=pltpu.CompilerParams(collective_id=0, has_side_effects=True, vmem_limit_bytes=67043328),
            name='decode_step',
        )(x, w_dq, g_q, w_uq, w_dkv.T, g_kv.reshape(1, latent), w_uk, w_uv, w_o,
          cache_c, jnp.swapaxes(cache_kr, 1, 2), jnp.asarray(freq), ctx_len)
        vspec = pl.BlockSpec(memory_space=pltpu.VMEM)
        return pl.pallas_call(split_outputs, out_shape=out_shape, in_specs=[vspec], out_specs=(vspec,) * 3,
                              name='split_outputs')(packed)

    spec_rows = P('dp', None)
    spec_cache = P('dp', 'cp', None)
    in_specs = (spec_rows, P(), P(), P(), P(), P(), P(), P(), P(), spec_cache, spec_cache, P('dp'))
    out_specs = (spec_rows, spec_rows, spec_rows)
    return jax.shard_map(decode_step, mesh=mesh, in_specs=in_specs, out_specs=out_specs, check_vma=False)
```

```python
import functools
import math

import jax
import jax.numpy as jnp
import numpy as np
from jax import lax
from jax.experimental import pallas as pl
from jax.experimental.pallas import tpu as pltpu
from jax.sharding import PartitionSpec as P

NORM_EPS = 1e-6
ROPE_THETA = 10000.0
MASKED = -1e30
FLOOR = -1e29
F32, BF16 = jnp.float32, jnp.bfloat16
MESH = pl.DeviceIdType.MESH
NT = (((1,), (1,)), ((), ()))
LANES = 128


def dot(a, b):
    return jnp.dot(a, b, preferred_element_type=F32)


def dot_nt(a, b):
    return lax.dot_general(a, b, NT, preferred_element_type=F32)


def rounded(v):
    return v.astype(BF16).astype(F32)


def wait_bytes(view, sem):
    pltpu.make_async_copy(view, view, sem).wait()


def step_kernel(dims, x_h, wdq_h, gq_h, wuq_h, wdkv_h, gkv_h, wuk_h, wuv_h, wo_h, cc_h, kr_h, freq_h, ctx_s,
                out_v,
                x_v, gq_v, wuq_v, wdkv_v, gkv_v, wuk_v, wuv_v, wo_v, cc_v, kr_v, freq_v, wv_v, wk_v, stage_v,
                xf_v, cq_v, kvp_v, q_v, cnf_v, sa_v, sb_v, m_v, acc_v, pair_v, xs_v, xsr_v, ys_v, ysr_v, olat_v, po_v, pop_v, pt_v, ptr_v, ag_v,
                in_sem, dq_sem, uq_sem, uk_sem, cc_sem,
                a_send, a_recv, kv_send, kv_recv, q_send, q_recv, pair_send, pair_recv, xs_send, xs_recv, ys_send, ys_recv,
                po_send, po_recv, pt_send, pt_recv, ag_send, ag_recv, ag2_send, ag2_recv):
    cp, side = dims
    chips = cp // 2
    inner = 2 * side
    nreq, dmodel = x_v.shape
    nslab, latent, slab, nope = wuk_v.shape
    half_heads = nslab * slab
    heads = 2 * half_heads
    rope = kr_v.shape[1]
    half_rope = rope // 2
    tdev = cc_v.shape[1]
    wide = latent + LANES
    qk = nope + rope
    kdkv = wdkv_v.shape[1]
    own = heads // cp

    d = lax.axis_index('cp')
    c = lax.rem(d, 2)
    t = d // 2
    oc = 1 - c
    gi = lax.rem(d, inner)
    base = d - gi
    xx = gi // 2
    yy = d // inner
    partner = base + 2 * xx + oc

    kstep = 64

    def widen(src):
        def go(i, _):
            r = pl.multiple_of(i * kstep, kstep)
            stage_v[pl.ds(pl.multiple_of(r * slab, kstep * slab), kstep * slab), :] = (
                src[pl.ds(r, kstep)].astype(F32).reshape(kstep * slab, nope))
            return 0
        lax.fori_loop(0, latent // kstep, go, 0)

    def chip_at(r):
        return lax.rem(t + r, chips)

    pending = {}

    def done(name):
        pending.pop(name)()

    def drain():
        for name in list(pending):
            done(name)

    def local(name, src, dst, sem):
        cpy = pltpu.make_async_copy(src, dst, sem)
        cpy.start()
        pending[name] = cpy.wait

    local('x', x_h, x_v, in_sem.at[0])
    nslot, krow, ucol = wuq_v.shape
    ndq = dmodel // krow
    for j in range(ndq):
        pltpu.make_async_copy(wdq_h.at[pl.ds(j * krow, krow), pl.ds(pl.multiple_of(c * ucol, LANES), ucol)],
                              wuq_v.at[j], dq_sem.at[j]).start()
    local('gq', gq_h, gq_v, in_sem.at[3])
    local('gkv', gkv_h, gkv_v, in_sem.at[4])
    local('freq', freq_h, freq_v, in_sem.at[5])
    nuq = wuq_h.shape[1] // 2 // ucol

    def uq_copy(j):
        return pltpu.make_async_copy(wuq_h.at[:, pl.ds(pl.multiple_of((c * nuq + j) * ucol, LANES), ucol)],
                                     wuq_v.at[lax.rem(ndq + j, nslot)], uq_sem.at[j])

    def uk_copy(s):
        return pltpu.make_async_copy(wuk_h.at[:, pl.ds(pl.multiple_of(c * half_heads + s * slab, slab), slab), :],
                                     wuk_v.at[s], uk_sem.at[s])

    def cache_copies(b):
        return (pltpu.make_async_copy(cc_h.at[b], cc_v.at[b], cc_sem.at[0, b]),
                pltpu.make_async_copy(kr_h.at[b], kr_v.at[b], cc_sem.at[1, b]))

    def cache_start(b):
        for cpy in cache_copies(b):
            cpy.start()

    def cache_wait(b):
        for cpy in cache_copies(b):
            cpy.wait()

    head0 = c * half_heads + xx * slab + yy * own
    head_slab = head0 // slab
    head_in = head0 - head_slab * slab

    barrier = pltpu.get_barrier_semaphore()

    def greet(r, _):
        pl.semaphore_signal(barrier, inc=1, device_id={'cp': 2 * chip_at(r) + c}, device_id_type=MESH)
        return 0

    lax.fori_loop(1, chips, greet, 0)
    for i in range(side):
        pl.semaphore_signal(barrier, inc=1, device_id={'cp': base + 2 * i + oc}, device_id_type=MESH)

    done('x')
    local('dkv', wdkv_h.at[:, pl.ds(pl.multiple_of(gi * kdkv, LANES), kdkv)], wdkv_v, in_sem.at[2])
    for s in range(nslab):
        uk_copy(s).start()

    def a_step(j, part):
        pltpu.make_async_copy(wuq_v.at[j], wuq_v.at[j], dq_sem.at[j]).wait()

        @pl.when(j >= 2)
        def _():
            uq_copy(j - 2).start()
        return part + dot(x_v[:, pl.ds(pl.multiple_of(j * krow, krow), krow)], wuq_v[j])

    part = lax.fori_loop(0, ndq, a_step, jnp.zeros((nreq, ucol), F32))
    cq_v[c] = part
    pl.semaphore_wait(barrier, chips - 1 + side)
    cq_copy = pltpu.make_async_remote_copy(src_ref=cq_v.at[c], dst_ref=cq_v.at[c], send_sem=a_send, recv_sem=a_recv,
                                           device_id={'cp': partner}, device_id_type=MESH)
    cq_copy.start()
    for j in range(ndq - 2, nslot - ndq):
        uq_copy(j).start()
    pending['cq'] = cq_copy.wait

    def to_ring(buf, send, recv):
        def go(r, _):
            peer = lax.rem(gi + r, inner)
            pltpu.make_async_remote_copy(src_ref=buf.at[gi], dst_ref=buf.at[gi], send_sem=send, recv_sem=recv,
                                         device_id={'cp': base + peer}, device_id_type=MESH).start()
            return 0
        lax.fori_loop(1, inner, go, 0)

    done('dkv')
    kvp_v[gi, :, 0:latent + rope] = dot_nt(x_v[:, pl.ds(pl.multiple_of(gi * kdkv, LANES), kdkv)], wdkv_v[...])
    kvp_v[gi, :, latent + rope:] = jnp.zeros((nreq, wide - latent - rope), F32)
    to_ring(kvp_v, kv_send, kv_recv)
    pending['kv_send'] = lambda: wait_bytes(kvp_v.at[pl.ds(0, inner - 1)], kv_send)
    pending['kv_recv'] = lambda: wait_bytes(kvp_v.at[pl.ds(0, inner - 1)], kv_recv)

    xall = x_v[...].astype(F32)
    for i in range(2):
        xf_v[i] = xall[4 * i:4 * i + 4, :]
    rows = lax.broadcasted_iota(jnp.int32, (nreq, LANES), 0)
    ctx = jnp.zeros((nreq, LANES), jnp.int32)
    for b in range(nreq):
        ctx = jnp.where(rows == b, ctx_s[b], ctx)
    done('freq')
    angles = ctx.astype(F32) * freq_v[...]
    cos_full = jnp.cos(angles)[:, :rope]
    sin_raw = jnp.sin(angles)[:, :rope]
    lane = lax.broadcasted_iota(jnp.int32, (nreq, rope), 1)
    sin_full = jnp.where(lane < half_rope, -sin_raw, sin_raw)

    def rope_rotate(v):
        swapped = jnp.concatenate([v[:, half_rope:], v[:, :half_rope]], axis=1)
        return v * cos_full + swapped * sin_full

    def uk_step(s, _):
        uk_copy(s).wait()
        uq_copy(nslot - ndq + s).start()
        widen(wuk_v.at[s])

        def head_step(i, _):
            wk_v[s * slab + i] = stage_v[pl.ds(i, latent, stride=slab), :].astype(BF16)
            return 0
        lax.fori_loop(0, slab, head_step, 0)
        return 0

    lax.fori_loop(0, nslab, uk_step, 0)

    done('cq')
    cq = rounded(jnp.concatenate([cq_v[0], cq_v[1]], axis=1))
    done('gq')
    mean_sq = jnp.mean(cq * cq, axis=1, keepdims=True)
    cn = (cq * lax.rsqrt(mean_sq + NORM_EPS) * gq_v[...].reshape(1, gq_v.shape[0])).astype(BF16)
    row0 = c * half_heads * nreq
    zeros_pad = jnp.zeros((nreq, LANES - rope), F32)
    per = ucol // qk

    def q_slab_copy(s):
        view = q_v.at[:, pl.ds(pl.multiple_of(row0 + s * slab * nreq, slab * nreq), slab * nreq)]
        return pltpu.make_async_remote_copy(src_ref=view, dst_ref=view, send_sem=q_send.at[s], recv_sem=q_recv.at[s],
                                            device_id={'cp': partner}, device_id_type=MESH)

    def q_latent(j, qc):
        for i in range(per):
            h = j * per + i
            r = pl.multiple_of(row0 + h * nreq, nreq)
            qr = rounded(rope_rotate(qc[:, i * qk + nope:(i + 1) * qk]))
            q_v[latent // LANES, pl.ds(r, nreq), :] = jnp.concatenate([qr, zeros_pad], axis=1)
            ql = rounded(dot_nt(qc[:, i * qk:i * qk + nope].astype(BF16), wk_v[h]))
            for k in range(latent // LANES):
                q_v[k, pl.ds(r, nreq), :] = ql[:, k * LANES:(k + 1) * LANES]
    def b_step(j, last):
        uq_copy(j).wait()
        cache_start(j - 1)
        qc = rounded(dot(cn, wuq_v[lax.rem(ndq + j, nslot)]))
        q_latent(j - 1, last)

        @pl.when(lax.rem(j * per, slab) == 0)
        def _():
            q_slab_copy(j * per // slab - 1).start()
        return qc

    uq_copy(0).wait()
    qc = lax.fori_loop(1, nuq, b_step, rounded(dot(cn, wuq_v[ndq])))
    cache_start(nuq - 1)
    q_latent(nuq - 1, qc)
    q_slab_copy(nslab - 1).start()
    for s in range(nslab):
        pending['q', s] = q_slab_copy(s).wait
    local('uv', wuv_h.at[:, pl.ds(pl.multiple_of(head_slab * slab, slab), slab), :], wuv_v, in_sem.at[6])
    local('wo', wo_h.at[pl.ds(pl.multiple_of(head0 * nope, own * nope), own * nope), :], wo_v, in_sem.at[7])

    done('kv_recv')
    kv = kvp_v[0]
    for i in range(1, inner):
        kv = kv + kvp_v[i]
    kvl = kv[:, :latent]
    done('gkv')
    mean_sq = jnp.mean(kvl * kvl, axis=1, keepdims=True)
    c_new = kvl * lax.rsqrt(mean_sq + NORM_EPS) * gkv_v[...]
    kr_new = rope_rotate(kv[:, latent:latent + rope])
    out_v[:, dmodel:dmodel + latent] = c_new.astype(BF16)
    out_v[:, dmodel + latent:] = jnp.concatenate([kr_new, zeros_pad], axis=1).astype(BF16)
    cnf_v[:, :latent] = rounded(c_new)
    cnf_v[:, latent:] = jnp.concatenate([rounded(kr_new), zeros_pad], axis=1)

    for s in range(nslab):
        done(('q', s))

    scale = (nope + rope) ** -0.5
    block0 = d * tdev
    head_row = lax.broadcasted_iota(jnp.int32, (heads, 1), 0)
    mine0 = pl.multiple_of(c * half_heads, half_heads)
    theirs0 = pl.multiple_of(oc * half_heads, half_heads)

    def pair_copy(b):
        return pltpu.make_async_remote_copy(src_ref=acc_v.at[b, pl.ds(theirs0, half_heads)], dst_ref=pair_v.at[b],
                                            send_sem=pair_send.at[b], recv_sem=pair_recv.at[b],
                                            device_id={'cp': partner}, device_id_type=MESH)

    nkc = 4
    kc = tdev // nkc
    half_lane = lax.broadcasted_iota(jnp.int32, (heads, LANES), 1) < LANES // 2
    chunk_pos = lax.broadcasted_iota(jnp.int32, (heads, kc), 1)

    def q_of(b):
        return jnp.concatenate([q_v[k, pl.ds(b, heads, stride=nreq), :] for k in range(wide // LANES)], axis=1)

    def scores(b, s_ref):
        qb = q_of(b).astype(BF16)
        left = ctx_s[b] - block0
        m = None
        for k in range(nkc):
            cols = slice(k * kc, (k + 1) * kc)
            s = (dot_nt(qb[:, :latent], cc_v[b, cols]) + dot(qb[:, latent:latent + rope], kr_v[b, :, cols])) * scale
            s = jnp.where(chunk_pos < left - k * kc, s, MASKED)
            s_ref[:, cols] = s
            mk = jnp.max(s, axis=1, keepdims=True)
            m = mk if m is None else jnp.maximum(m, mk)
        m_v[b] = jnp.broadcast_to(m, (heads, LANES))

    def weigh(b, s_ref):
        qf = q_of(b)
        left = ctx_s[b] - block0
        new_row = cnf_v[pl.ds(b, 1), :]
        new_s = jnp.sum(qf * new_row, axis=1, keepdims=True) * scale
        at = head_row * 0 + left
        new_s = jnp.where(jnp.logical_and(at >= 0, at < tdev), new_s, MASKED)
        m = jnp.maximum(jnp.maximum(m_v[b][:, :1], new_s), FLOOR)
        new_w = jnp.exp(new_s - m)
        l = new_w
        acc = rounded(new_w) * new_row[:, :latent]
        for k in range(nkc):
            cols = slice(k * kc, (k + 1) * kc)
            p = jnp.exp(s_ref[:, cols] - m)
            l = l + jnp.sum(p, axis=1, keepdims=True)
            acc = acc + dot(p.astype(BF16), cc_v[b, cols])
        acc_v[b, :, :latent] = acc
        acc_v[b, :, latent:] = jnp.where(half_lane, m, l)

    quarter = half_heads // side

    def ring_peer(axis, r):
        if axis == 0:
            p = lax.rem(xx + r, side)
            return p, base + 2 * p + c
        p = lax.rem(yy + r, side)
        return p, p * inner + gi

    here = (xx, yy)

    def xs_copy(b, axis, r):
        p, dev = ring_peer(axis, r)
        return pltpu.make_async_remote_copy(src_ref=xs_v.at[b, pl.ds(pl.multiple_of(p * quarter, quarter), quarter)],
                                            dst_ref=xsr_v.at[b, r - 1], send_sem=xs_send.at[b], recv_sem=xs_recv.at[b],
                                            device_id={'cp': dev}, device_id_type=MESH)

    def ys_copy(b, axis, r):
        p, dev = ring_peer(1 - axis, r)
        return pltpu.make_async_remote_copy(src_ref=ys_v.at[b, p], dst_ref=ysr_v.at[b, r - 1],
                                            send_sem=ys_send.at[b], recv_sem=ys_recv.at[b],
                                            device_id={'cp': dev}, device_id_type=MESH)

    def ml_of(v):
        return v[:, latent:latent + 1], v[:, wide - 1:wide]

    def merge(parts):
        ms, ls = zip(*[ml_of(p) for p in parts])
        m = functools.reduce(jnp.maximum, ms)
        fs = [jnp.exp(mi - m) for mi in ms]
        l = sum(f * li for f, li in zip(fs, ls))
        acc = sum(f * p[:, :latent] for f, p in zip(fs, parts))
        return m, l, acc

    def with_ml(m, l):
        side_lane = lax.broadcasted_iota(jnp.int32, (m.shape[0], LANES), 1)
        return jnp.where(side_lane < LANES // 2, m, l)

    def pair_step(b, axis):
        pair_copy(b).wait_recv()
        m, l, acc = merge([acc_v[b, pl.ds(mine0, half_heads), :], pair_v[b]])
        ml = with_ml(m, l)
        if axis == 0:
            xs_v[b, :, :latent] = acc
            xs_v[b, :, latent:] = ml
        else:
            for p in range(side):
                for k in range(side):
                    src = slice(p * quarter + k * own, p * quarter + (k + 1) * own)
                    dst = slice(k * quarter + p * own, k * quarter + (p + 1) * own)
                    xs_v[b, dst, :latent] = acc[src]
                    xs_v[b, dst, latent:] = ml[src]
        for r in range(1, side):
            xs_copy(b, axis, r).start()

    def ring_merge(b, axis):
        mine = xs_v[b, pl.ds(pl.multiple_of(here[axis] * quarter, quarter), quarter), :]
        m, l, acc = merge([mine] + [xsr_v[b, r] for r in range(side - 1)])
        ml = with_ml(m, l)
        for k in range(side):
            ys_v[b, k, :, :latent] = acc[own * k:own * (k + 1), :]
            ys_v[b, k, :, latent:] = ml[own * k:own * (k + 1), :]

    def two_requests(i, _):
        b = 2 * i
        cache_wait(b + 1)
        scores(b + 1, sb_v)
        weigh(b, sa_v)
        pair_copy(b).start()

        @pl.when(i > 0)
        def _():
            pair_step(b - 1, 1)

        @pl.when(b + 2 < nreq)
        def _():
            cache_wait(b + 2)
        scores(jnp.minimum(b + 2, nreq - 1), sa_v)
        weigh(b + 1, sb_v)
        pair_copy(b + 1).start()
        pair_step(b, 0)
        return 0

    cache_wait(0)
    scores(0, sa_v)
    lax.fori_loop(0, nreq // 2, two_requests, 0)
    for b in range(nreq):
        pending['pair', b] = pair_copy(b).wait_send

    def ring_step(i, _):
        for k in range(2):
            wait_bytes(xsr_v.at[2 * i + k], xs_recv.at[2 * i + k])
        for k in range(2):
            ring_merge(2 * i + k, k)
        for k in range(2):
            for r in range(1, side):
                ys_copy(2 * i + k, k, r).start()
        return 0

    lax.fori_loop(0, 1, ring_step, 0)
    pair_step(nreq - 1, 1)
    lax.fori_loop(1, nreq // 2, ring_step, 0)

    def each(view, sem):
        def go(b, _):
            wait_bytes(view.at[b], sem.at[b])
            return 0
        return lambda: lax.fori_loop(0, nreq, go, 0)

    pending['xs_send'] = each(xsr_v, xs_send)
    pending['ys_send'] = each(ysr_v, ys_send)
    pending['ys_recv'] = each(ysr_v, ys_recv)

    done('uv')
    widen(wuv_v)
    for k in range(own):
        wv_v[k] = stage_v[pl.ds(head_in + k, latent, stride=slab), :].astype(BF16)

    done('ys_recv')
    for b in range(nreq):
        m, l, acc = merge([ys_v[b, here[1 - b % 2]]] + [ysr_v[b, r] for r in range(side - 1)])
        ol = rounded(acc / l)
        for k in range(own):
            olat_v[k, b:b + 1, :] = ol[k:k + 1, :]

    done('wo')
    outs = []
    for k in range(own):
        outs.append(dot(olat_v[k].astype(BF16), wv_v[k]).astype(BF16))
    o = jnp.concatenate(outs, axis=1)
    ncol = 768
    for j in range(dmodel // ncol):
        pj = dot(o, wo_v[:, j * ncol:(j + 1) * ncol])
        for i in range(2):
            po_v[i, :, j * ncol:(j + 1) * ncol] = pj[4 * i:4 * i + 4, :]
    po_copy = pltpu.make_async_remote_copy(src_ref=po_v.at[oc], dst_ref=pop_v, send_sem=po_send, recv_sem=po_recv,
                                           device_id={'cp': partner}, device_id_type=MESH)
    po_copy.start()
    po_copy.wait()
    tcol = dmodel // chips
    for k in range(chips):
        pt_v[k] = po_v[c, :, k * tcol:(k + 1) * tcol] + pop_v[:, k * tcol:(k + 1) * tcol]

    def pt_go(r, _):
        pltpu.make_async_remote_copy(src_ref=pt_v.at[chip_at(r)], dst_ref=ptr_v.at[r - 1], send_sem=pt_send, recv_sem=pt_recv,
                                     device_id={'cp': 2 * chip_at(r) + c}, device_id_type=MESH).start()
        return 0
    lax.fori_loop(1, chips, pt_go, 0)
    pending['pt_send'] = lambda: wait_bytes(ptr_v, pt_send)
    wait_bytes(ptr_v, pt_recv)
    tot = pt_v[t]
    for r in range(chips - 1):
        tot = tot + ptr_v[r]
    ag_v[c, t] = rounded(xf_v[c, :, pl.ds(pl.multiple_of(t * tcol, LANES), tcol)] + tot)

    def ag_go(r, _):
        pltpu.make_async_remote_copy(src_ref=ag_v.at[c, t], dst_ref=ag_v.at[c, t], send_sem=ag_send, recv_sem=ag_recv,
                                     device_id={'cp': 2 * chip_at(r) + c}, device_id_type=MESH).start()
        return 0
    lax.fori_loop(1, chips, ag_go, 0)
    pending['ag_send'] = lambda: wait_bytes(ag_v.at[0, pl.ds(0, chips - 1)], ag_send)
    wait_bytes(ag_v.at[0, pl.ds(0, chips - 1)], ag_recv)
    ag_copy = pltpu.make_async_remote_copy(src_ref=ag_v.at[c], dst_ref=ag_v.at[c], send_sem=ag2_send, recv_sem=ag2_recv,
                                           device_id={'cp': partner}, device_id_type=MESH)
    ag_copy.start()
    ag_copy.wait()
    for k in range(chips):
        out_v[:, k * tcol:(k + 1) * tcol] = jnp.concatenate([ag_v[0, k], ag_v[1, k]], axis=0).astype(BF16)

    drain()


def split_outputs(packed_v, xo_v, cn_v, kr_v):
    dmodel, latent, rope = xo_v.shape[1], cn_v.shape[1], kr_v.shape[1]
    xo_v[...] = packed_v[:, :dmodel]
    cn_v[...] = packed_v[:, dmodel:dmodel + latent]
    kr_v[...] = packed_v[:, dmodel + latent:dmodel + latent + rope]


def solution(mesh):
    cp = mesh.shape['cp']
    side = math.isqrt(cp // 2)
    inner = 2 * side
    chips = cp // 2

    def decode_step(x, w_dq, g_q, w_uq, w_dkv, g_kv, w_uk, w_uv, w_o, cache_c, cache_kr, ctx_len):
        nreq, dmodel = x.shape
        qlora = w_dq.shape[1]
        latent, heads, nope = w_uk.shape
        rope = cache_kr.shape[2]
        tdev = cache_c.shape[1]
        half = heads // 2
        own = heads // cp
        wide = latent + LANES
        tcol = dmodel // chips
        inv = (np.float64(ROPE_THETA) ** (-2.0 * np.arange(rope // 2) / rope)).astype(np.float32)
        freq = np.zeros((1, LANES), np.float32)
        freq[0, :rope] = np.concatenate([inv, inv])
        anyspec = pl.BlockSpec(memory_space=pl.ANY)
        dma = pltpu.SemaphoreType.DMA
        vm = pltpu.VMEM
        out_shape = (jax.ShapeDtypeStruct((nreq, dmodel), BF16), jax.ShapeDtypeStruct((nreq, latent), BF16),
                     jax.ShapeDtypeStruct((nreq, rope), BF16))
        scratch = [
            vm((nreq, dmodel), BF16), vm((qlora,), F32),
            vm((w_uq.shape[1] // qlora, qlora, qlora // 2), BF16), vm((w_dkv.shape[1], dmodel // inner), BF16), vm((1, latent), F32),
            vm((half // 8, latent, 8, nope), BF16), vm((latent, 8, nope), BF16), vm((own * nope, dmodel), BF16),
            vm((nreq, tdev, latent), BF16), vm((nreq, rope, tdev), BF16), vm((1, LANES), F32), vm((own, latent, nope), BF16),
            vm((half, latent, nope), BF16), vm((latent * 8, nope), F32),
            vm((2, nreq // 2, dmodel), F32), vm((2, nreq, qlora // 2), F32), vm((inner, nreq, wide), F32),
            vm((wide // LANES, heads * nreq, LANES), F32), vm((nreq, wide), F32),
            vm((heads, tdev), F32), vm((heads, tdev), F32), vm((nreq, heads, LANES), F32),
            vm((nreq, heads, wide), F32), vm((nreq, half, wide), F32),
            vm((nreq, half, wide), F32), vm((nreq, side - 1, half // side, wide), F32),
            vm((nreq, side, own, wide), F32), vm((nreq, side - 1, own, wide), F32), vm((own, nreq, latent), F32),
            vm((2, nreq // 2, dmodel), F32), vm((nreq // 2, dmodel), F32),
            vm((chips, nreq // 2, tcol), F32), vm((chips - 1, nreq // 2, tcol), F32), vm((2, chips, nreq // 2, tcol), F32),
            dma((8,)), dma((dmodel // qlora,)), dma((w_uq.shape[1] // qlora,)), dma((half // 8,)), dma((2, nreq)),
            dma, dma, dma, dma, dma((half // 8,)), dma((half // 8,)), dma((nreq,)), dma((nreq,)), dma((nreq,)), dma((nreq,)), dma((nreq,)), dma((nreq,)),
            dma, dma, dma, dma, dma, dma, dma, dma,
        ]
        packed = pl.pallas_call(
            functools.partial(step_kernel, (cp, side)),
            out_shape=jax.ShapeDtypeStruct((nreq, dmodel + wide), BF16),
            in_specs=[anyspec] * 12 + [pl.BlockSpec(memory_space=pltpu.SMEM)],
            out_specs=pl.BlockSpec(memory_space=pltpu.VMEM),
            scratch_shapes=scratch,
            compiler_params=pltpu.CompilerParams(collective_id=0, has_side_effects=True, vmem_limit_bytes=67043328),
            name='decode_step',
        )(x, w_dq, g_q, w_uq, w_dkv.T, g_kv.reshape(1, latent), w_uk, w_uv, w_o,
          cache_c, jnp.swapaxes(cache_kr, 1, 2), jnp.asarray(freq), ctx_len)
        vspec = pl.BlockSpec(memory_space=pltpu.VMEM)
        return pl.pallas_call(split_outputs, out_shape=out_shape, in_specs=[vspec], out_specs=(vspec,) * 3,
                              name='split_outputs')(packed)

    spec_rows = P('dp', None)
    spec_cache = P('dp', 'cp', None)
    in_specs = (spec_rows, P(), P(), P(), P(), P(), P(), P(), P(), spec_cache, spec_cache, P('dp'))
    out_specs = (spec_rows, spec_rows, spec_rows)
    return jax.shard_map(decode_step, mesh=mesh, in_specs=in_specs, out_specs=out_specs, check_vma=False)
```

```python
import functools
import math

import jax
import jax.numpy as jnp
import numpy as np
from jax import lax
from jax.experimental import pallas as pl
from jax.experimental.pallas import tpu as pltpu
from jax.sharding import PartitionSpec as P

NORM_EPS = 1e-6
ROPE_THETA = 10000.0
MASKED = -1e30
FLOOR = -1e29
F32, BF16 = jnp.float32, jnp.bfloat16
MESH = pl.DeviceIdType.MESH
NT = (((1,), (1,)), ((), ()))
LANES = 128


def dot(a, b):
    return jnp.dot(a, b, preferred_element_type=F32)


def dot_nt(a, b):
    return lax.dot_general(a, b, NT, preferred_element_type=F32)


def rounded(v):
    return v.astype(BF16).astype(F32)


def wait_bytes(view, sem):
    pltpu.make_async_copy(view, view, sem).wait()


def step_kernel(dims, x_h, wdq_h, gq_h, wuq_h, wdkv_h, gkv_h, wuk_h, wuv_h, wo_h, cc_h, kr_h, freq_h, ctx_s,
                out_v,
                x_v, gq_v, wuq_v, wdkv_v, gkv_v, wuk_v, wuv_v, wo_v, cc_v, kr_v, freq_v, wv_v, wk_v, stage_v,
                xf_v, cq_v, kvp_v, q_v, cnf_v, sa_v, sb_v, ma_v, mb_v, acc_v, pair_v, xs_v, xsr_v, ys_v, ysr_v, rs_v, rsr_v, olat_v, po_v, pop_v, pt_v, ptr_v, ag_v,
                in_sem, dq_sem, uq_sem, uk_sem, cc_sem,
                a_send, a_recv, kv_send, kv_recv, q_send, q_recv, pair_send, pair_recv, xs_send, xs_recv, ys_send, ys_recv, rs_send, rs_recv,
                po_send, po_recv, pt_send, pt_recv, ag_send, ag_recv, ag2_send, ag2_recv):
    cp, side = dims
    chips = cp // 2
    inner = 2 * side
    nreq, dmodel = x_v.shape
    nslab, latent, slab, nope = wuk_v.shape
    half_heads = nslab * slab
    heads = 2 * half_heads
    rope = kr_v.shape[1]
    half_rope = rope // 2
    tdev = cc_v.shape[1]
    wide = latent + LANES
    qk = nope + rope
    kdkv = wdkv_v.shape[1]
    own = heads // cp

    d = lax.axis_index('cp')
    c = lax.rem(d, 2)
    t = d // 2
    oc = 1 - c
    gi = lax.rem(d, inner)
    base = d - gi
    xx = gi // 2
    yy = d // inner
    partner = base + 2 * xx + oc

    kstep = 64

    def widen(src):
        def go(i, _):
            r = pl.multiple_of(i * kstep, kstep)
            stage_v[pl.ds(pl.multiple_of(r * slab, kstep * slab), kstep * slab), :] = (
                src[pl.ds(r, kstep)].astype(F32).reshape(kstep * slab, nope))
            return 0
        lax.fori_loop(0, latent // kstep, go, 0)

    def chip_at(r):
        return lax.rem(t + r, chips)

    pending = {}

    def done(name):
        pending.pop(name)()

    def drain():
        for name in list(pending):
            done(name)

    def local(name, src, dst, sem):
        cpy = pltpu.make_async_copy(src, dst, sem)
        cpy.start()
        pending[name] = cpy.wait

    local('x', x_h, x_v, in_sem.at[0])
    nslot, krow, ucol = wuq_v.shape
    ndq = dmodel // krow
    local('gq', gq_h, gq_v, in_sem.at[3])
    local('gkv', gkv_h, gkv_v, in_sem.at[4])
    local('freq', freq_h, freq_v, in_sem.at[5])
    nuq = wuq_h.shape[1] // 2 // ucol

    def uq_copy(j):
        return pltpu.make_async_copy(wuq_h.at[:, pl.ds(pl.multiple_of((c * nuq + j) * ucol, LANES), ucol)],
                                     wuq_v.at[lax.rem(ndq + j, nslot)], uq_sem.at[j])

    def uk_copy(s):
        return pltpu.make_async_copy(wuk_h.at[:, pl.ds(pl.multiple_of(c * half_heads + s * slab, slab), slab), :],
                                     wuk_v.at[s], uk_sem.at[s])

    def cache_copies(b):
        return (pltpu.make_async_copy(cc_h.at[b], cc_v.at[b], cc_sem.at[0, b]),
                pltpu.make_async_copy(kr_h.at[b], kr_v.at[b], cc_sem.at[1, b]))

    def cache_start(b):
        for cpy in cache_copies(b):
            cpy.start()

    def cache_wait(b):
        for cpy in cache_copies(b):
            cpy.wait()

    head0 = c * half_heads + xx * slab + yy * own
    head_slab = head0 // slab
    head_in = head0 - head_slab * slab

    for s in range(nslab):
        uk_copy(s).start()
    for j in range(ndq):
        pltpu.make_async_copy(wdq_h.at[pl.ds(j * krow, krow), pl.ds(pl.multiple_of(c * ucol, LANES), ucol)],
                              wuq_v.at[j], dq_sem.at[j]).start()
    local('dkv', wdkv_h.at[:, pl.ds(pl.multiple_of(gi * kdkv, LANES), kdkv)], wdkv_v, in_sem.at[2])

    barrier = pltpu.get_barrier_semaphore()

    def greet(r, _):
        pl.semaphore_signal(barrier, inc=1, device_id={'cp': 2 * chip_at(r) + c}, device_id_type=MESH)
        return 0

    lax.fori_loop(1, chips, greet, 0)
    for i in range(side):
        pl.semaphore_signal(barrier, inc=1, device_id={'cp': base + 2 * i + oc}, device_id_type=MESH)

    def uk_step(s, _):
        uk_copy(s).wait()
        widen(wuk_v.at[s])

        def head_step(i, _):
            wk_v[s * slab + i] = stage_v[pl.ds(i, latent, stride=slab), :].astype(BF16)
            return 0
        lax.fori_loop(0, slab, head_step, 0)
        return 0

    lax.fori_loop(0, nslab, uk_step, 0)
    for j in range(2):
        uq_copy(j).start()

    done('x')
    def a_step(j, part):
        pltpu.make_async_copy(wuq_v.at[j], wuq_v.at[j], dq_sem.at[j]).wait()

        @pl.when(j < nslot - ndq - 2)
        def _():
            uq_copy(j + 2).start()
        return part + dot(x_v[:, pl.ds(pl.multiple_of(j * krow, krow), krow)], wuq_v[j])

    part = lax.fori_loop(0, ndq, a_step, jnp.zeros((nreq, ucol), F32))
    cq_v[c] = part
    pl.semaphore_wait(barrier, chips - 1 + side)
    cq_copy = pltpu.make_async_remote_copy(src_ref=cq_v.at[c], dst_ref=cq_v.at[c], send_sem=a_send, recv_sem=a_recv,
                                           device_id={'cp': partner}, device_id_type=MESH)
    cq_copy.start()
    for j in range(nslot - ndq, nuq):
        uq_copy(j).start()
    pending['cq'] = cq_copy.wait

    def to_ring(buf, send, recv):
        def go(r, _):
            peer = lax.rem(gi + r, inner)
            pltpu.make_async_remote_copy(src_ref=buf.at[gi], dst_ref=buf.at[gi], send_sem=send, recv_sem=recv,
                                         device_id={'cp': base + peer}, device_id_type=MESH).start()
            return 0
        lax.fori_loop(1, inner, go, 0)

    done('dkv')
    kvp_v[gi, :, 0:latent + rope] = dot_nt(x_v[:, pl.ds(pl.multiple_of(gi * kdkv, LANES), kdkv)], wdkv_v[...])
    kvp_v[gi, :, latent + rope:] = jnp.zeros((nreq, wide - latent - rope), F32)
    to_ring(kvp_v, kv_send, kv_recv)
    pending['kv_send'] = lambda: wait_bytes(kvp_v.at[pl.ds(0, inner - 1)], kv_send)
    pending['kv_recv'] = lambda: wait_bytes(kvp_v.at[pl.ds(0, inner - 1)], kv_recv)

    xall = x_v[...].astype(F32)
    for i in range(2):
        xf_v[i] = xall[4 * i:4 * i + 4, :]
    rows = lax.broadcasted_iota(jnp.int32, (nreq, LANES), 0)
    ctx = jnp.zeros((nreq, LANES), jnp.int32)
    for b in range(nreq):
        ctx = jnp.where(rows == b, ctx_s[b], ctx)
    done('freq')
    angles = ctx.astype(F32) * freq_v[...]
    cos_full = jnp.cos(angles)[:, :rope]
    sin_raw = jnp.sin(angles)[:, :rope]
    lane = lax.broadcasted_iota(jnp.int32, (nreq, rope), 1)
    sin_full = jnp.where(lane < half_rope, -sin_raw, sin_raw)

    def rope_rotate(v):
        swapped = jnp.concatenate([v[:, half_rope:], v[:, :half_rope]], axis=1)
        return v * cos_full + swapped * sin_full

    done('cq')
    cq = rounded(jnp.concatenate([cq_v[0], cq_v[1]], axis=1))
    done('gq')
    mean_sq = jnp.mean(cq * cq, axis=1, keepdims=True)
    cn = (cq * lax.rsqrt(mean_sq + NORM_EPS) * gq_v[...].reshape(1, gq_v.shape[0])).astype(BF16)
    row0 = c * half_heads * nreq
    zeros_pad = jnp.zeros((nreq, LANES - rope), F32)
    per = ucol // qk

    def q_slab_copy(s):
        view = q_v.at[:, pl.ds(pl.multiple_of(row0 + s * slab * nreq, slab * nreq), slab * nreq)]
        return pltpu.make_async_remote_copy(src_ref=view, dst_ref=view, send_sem=q_send.at[s], recv_sem=q_recv.at[s],
                                            device_id={'cp': partner}, device_id_type=MESH)

    def q_latent(j, qc):
        for i in range(per):
            h = j * per + i
            r = pl.multiple_of(row0 + h * nreq, nreq)
            qr = rounded(rope_rotate(qc[:, i * qk + nope:(i + 1) * qk]))
            q_v[latent // LANES, pl.ds(r, nreq), :] = jnp.concatenate([qr, zeros_pad], axis=1)
            ql = rounded(dot_nt(qc[:, i * qk:i * qk + nope].astype(BF16), wk_v[h]))
            for k in range(latent // LANES):
                q_v[k, pl.ds(r, nreq), :] = ql[:, k * LANES:(k + 1) * LANES]
    def b_step(j, last):
        uq_copy(j).wait()
        cache_start(j - 1)
        qc = rounded(dot(cn, wuq_v[lax.rem(ndq + j, nslot)]))
        q_latent(j - 1, last)

        @pl.when(lax.rem(j * per, slab) == 0)
        def _():
            q_slab_copy(j * per // slab - 1).start()
        return qc

    uq_copy(0).wait()
    qc = lax.fori_loop(1, nuq, b_step, rounded(dot(cn, wuq_v[ndq])))
    cache_start(nuq - 1)
    q_latent(nuq - 1, qc)
    q_slab_copy(nslab - 1).start()
    for s in range(nslab):
        pending['q', s] = q_slab_copy(s).wait
    local('uv', wuv_h.at[:, pl.ds(pl.multiple_of(head_slab * slab, slab), slab), :], wuv_v, in_sem.at[6])
    local('wo', wo_h.at[pl.ds(pl.multiple_of(head0 * nope, own * nope), own * nope), :], wo_v, in_sem.at[7])

    done('kv_recv')
    kv = kvp_v[0]
    for i in range(1, inner):
        kv = kv + kvp_v[i]
    kvl = kv[:, :latent]
    done('gkv')
    mean_sq = jnp.mean(kvl * kvl, axis=1, keepdims=True)
    c_new = kvl * lax.rsqrt(mean_sq + NORM_EPS) * gkv_v[...]
    kr_new = rope_rotate(kv[:, latent:latent + rope])
    out_v[:, dmodel:dmodel + latent] = c_new.astype(BF16)
    out_v[:, dmodel + latent:] = jnp.concatenate([kr_new, zeros_pad], axis=1).astype(BF16)
    cnf_v[:, :latent] = rounded(c_new)
    cnf_v[:, latent:] = jnp.concatenate([rounded(kr_new), zeros_pad], axis=1)

    for s in range(nslab):
        done(('q', s))

    scale = (nope + rope) ** -0.5
    block0 = d * tdev
    head_row = lax.broadcasted_iota(jnp.int32, (heads, 1), 0)
    mine0 = pl.multiple_of(c * half_heads, half_heads)
    theirs0 = pl.multiple_of(oc * half_heads, half_heads)

    def pair_copy(b):
        return pltpu.make_async_remote_copy(src_ref=acc_v.at[b, pl.ds(theirs0, half_heads)], dst_ref=pair_v.at[b],
                                            send_sem=pair_send.at[b], recv_sem=pair_recv.at[b],
                                            device_id={'cp': partner}, device_id_type=MESH)

    nkc = 4
    kc = tdev // nkc
    half_lane = lax.broadcasted_iota(jnp.int32, (heads, LANES), 1) < LANES // 2
    chunk_pos = lax.broadcasted_iota(jnp.int32, (heads, kc), 1)

    def q_of(b):
        return jnp.concatenate([q_v[k, pl.ds(b, heads, stride=nreq), :] for k in range(wide // LANES)], axis=1)

    def scores(b, s_ref, m_ref):
        qb = q_of(b).astype(BF16)
        left = ctx_s[b] - block0
        m = None
        for k in range(nkc):
            cols = slice(k * kc, (k + 1) * kc)
            s = (dot_nt(qb[:, :latent], cc_v[b, cols]) + dot(qb[:, latent:latent + rope], kr_v[b, :, cols])) * scale
            s = jnp.where(chunk_pos < left - k * kc, s, MASKED)
            s_ref[:, cols] = s
            mk = jnp.max(s, axis=1, keepdims=True)
            m = mk if m is None else jnp.maximum(m, mk)
        m_ref[...] = jnp.broadcast_to(m, (heads, LANES))

    def weigh(b, s_ref, m_ref):
        qf = q_of(b)
        left = ctx_s[b] - block0
        new_row = cnf_v[pl.ds(b, 1), :]
        new_s = jnp.sum(qf * new_row, axis=1, keepdims=True) * scale
        at = head_row * 0 + left
        new_s = jnp.where(jnp.logical_and(at >= 0, at < tdev), new_s, MASKED)
        m = jnp.maximum(jnp.maximum(m_ref[:, :1], new_s), FLOOR)
        new_w = jnp.exp(new_s - m)
        l = new_w
        acc = rounded(new_w) * new_row[:, :latent]
        for k in range(nkc):
            cols = slice(k * kc, (k + 1) * kc)
            p = jnp.exp(s_ref[:, cols] - m)
            l = l + jnp.sum(p, axis=1, keepdims=True)
            acc = acc + dot(p.astype(BF16), cc_v[b, cols])
        acc_v[b, :, :latent] = acc
        acc_v[b, :, latent:] = jnp.where(half_lane, m, l)

    quarter = half_heads // side

    def ring_peer(axis, r):
        if axis == 0:
            p = lax.rem(xx + r, side)
            return p, base + 2 * p + c
        p = lax.rem(yy + r, side)
        return p, p * inner + gi

    here = (xx, yy)

    def xs_copy(b, axis, r):
        p, dev = ring_peer(axis, r)
        return pltpu.make_async_remote_copy(src_ref=xs_v.at[b, pl.ds(pl.multiple_of(p * quarter, quarter), quarter)],
                                            dst_ref=xsr_v.at[b, r - 1], send_sem=xs_send.at[b], recv_sem=xs_recv.at[b],
                                            device_id={'cp': dev}, device_id_type=MESH)

    def ys_copy(b, axis, r):
        p, dev = ring_peer(1 - axis, r)
        return pltpu.make_async_remote_copy(src_ref=ys_v.at[b, p], dst_ref=ysr_v.at[b, r - 1],
                                            send_sem=ys_send.at[b], recv_sem=ys_recv.at[b],
                                            device_id={'cp': dev}, device_id_type=MESH)

    def ml_of(v):
        return v[:, latent:latent + 1], v[:, wide - 1:wide]

    def merge(parts):
        ms, ls = zip(*[ml_of(p) for p in parts])
        m = functools.reduce(jnp.maximum, ms)
        fs = [jnp.exp(mi - m) for mi in ms]
        l = sum(f * li for f, li in zip(fs, ls))
        acc = sum(f * p[:, :latent] for f, p in zip(fs, parts))
        return m, l, acc

    def with_ml(m, l):
        side_lane = lax.broadcasted_iota(jnp.int32, (m.shape[0], LANES), 1)
        return jnp.where(side_lane < LANES // 2, m, l)

    nring = nreq // 2

    def rs_copy(b, r):
        p = chip_at(r)
        return pltpu.make_async_remote_copy(src_ref=rs_v.at[b - nring, lax.rem(p, side) * side + p // side],
                                            dst_ref=rsr_v.at[b - nring, r - 1],
                                            send_sem=rs_send.at[b - nring], recv_sem=rs_recv.at[b - nring],
                                            device_id={'cp': 2 * p + c}, device_id_type=MESH)

    def direct_step(b):
        pair_copy(b).wait_recv()
        m, l, acc = merge([acc_v[b, pl.ds(mine0, half_heads), :], pair_v[b]])
        ml = with_ml(m, l)
        for k in range(chips):
            rs_v[b - nring, k, :, :latent] = acc[own * k:own * (k + 1), :]
            rs_v[b - nring, k, :, latent:] = ml[own * k:own * (k + 1), :]

        def go(r, _):
            rs_copy(b, r).start()
            return 0
        lax.fori_loop(1, chips, go, 0)

    def pair_step(b, axis):
        pair_copy(b).wait_recv()
        m, l, acc = merge([acc_v[b, pl.ds(mine0, half_heads), :], pair_v[b]])
        ml = with_ml(m, l)
        if axis == 0:
            xs_v[b, :, :latent] = acc
            xs_v[b, :, latent:] = ml
        else:
            for p in range(side):
                for k in range(side):
                    src = slice(p * quarter + k * own, p * quarter + (k + 1) * own)
                    dst = slice(k * quarter + p * own, k * quarter + (p + 1) * own)
                    xs_v[b, dst, :latent] = acc[src]
                    xs_v[b, dst, latent:] = ml[src]
        for r in range(1, side):
            xs_copy(b, axis, r).start()

    def ring_merge(b, axis):
        mine = xs_v[b, pl.ds(pl.multiple_of(here[axis] * quarter, quarter), quarter), :]
        m, l, acc = merge([mine] + [xsr_v[b, r] for r in range(side - 1)])
        ml = with_ml(m, l)
        for k in range(side):
            ys_v[b, k, :, :latent] = acc[own * k:own * (k + 1), :]
            ys_v[b, k, :, latent:] = ml[own * k:own * (k + 1), :]

    def ring_step(i):
        for k in range(2):
            wait_bytes(xsr_v.at[2 * i + k], xs_recv.at[2 * i + k])
        for k in range(2):
            ring_merge(2 * i + k, k)
        for k in range(2):
            for r in range(1, side):
                ys_copy(2 * i + k, k, r).start()

    def two_requests(i, _):
        b = 2 * i
        cache_wait(b + 1)
        scores(b + 1, sb_v, mb_v)
        weigh(b, sa_v, ma_v)
        pair_copy(b).start()

        @pl.when(jnp.logical_and(b - 1 > 0, b - 1 < nring))
        def _():
            pair_step(b - 1, 1)

        @pl.when(b - 1 >= nring)
        def _():
            direct_step(b - 1)

        @pl.when(b + 2 < nreq)
        def _():
            cache_wait(b + 2)
        scores(jnp.minimum(b + 2, nreq - 1), sa_v, ma_v)
        weigh(b + 1, sb_v, mb_v)
        pair_copy(b + 1).start()
        @pl.when(b < nring)
        def _():
            pair_step(b, 0)

        @pl.when(b >= nring)
        def _():
            direct_step(b)
            ring_step(i - nring // 2)
        return 0

    cache_wait(0)
    scores(0, sa_v, ma_v)
    lax.fori_loop(0, nreq // 2, two_requests, 0)
    for b in range(nreq):
        pending['pair', b] = pair_copy(b).wait_send

    direct_step(nreq - 1)

    def each(view, sem):
        def go(b, _):
            wait_bytes(view.at[b], sem.at[b])
            return 0
        return lambda: lax.fori_loop(0, nring, go, 0)

    pending['xs_send'] = each(xsr_v, xs_send)
    pending['ys_send'] = each(ysr_v, ys_send)
    pending['ys_recv'] = each(ysr_v, ys_recv)
    pending['rs_send'] = each(rsr_v, rs_send)
    pending['rs_recv'] = each(rsr_v, rs_recv)

    done('uv')
    widen(wuv_v)
    for k in range(own):
        wv_v[k] = stage_v[pl.ds(head_in + k, latent, stride=slab), :].astype(BF16)

    def put(b, acc, l):
        ol = rounded(acc / l)
        for k in range(own):
            olat_v[k, b:b + 1, :] = ol[k:k + 1, :]

    done('ys_recv')
    for b in range(nring):
        m, l, acc = merge([ys_v[b, here[1 - b % 2]]] + [ysr_v[b, r] for r in range(side - 1)])
        put(b, acc, l)
    done('rs_recv')
    for b in range(nring):
        m, l, acc = merge([rs_v[b, xx * side + yy]] + [rsr_v[b, r] for r in range(chips - 1)])
        put(nring + b, acc, l)

    done('wo')
    outs = []
    for k in range(own):
        outs.append(dot(olat_v[k].astype(BF16), wv_v[k]).astype(BF16))
    o = jnp.concatenate(outs, axis=1)
    ncol = 768
    for j in range(dmodel // ncol):
        pj = dot(o, wo_v[:, j * ncol:(j + 1) * ncol])
        for i in range(2):
            po_v[i, :, j * ncol:(j + 1) * ncol] = pj[4 * i:4 * i + 4, :]
    po_copy = pltpu.make_async_remote_copy(src_ref=po_v.at[oc], dst_ref=pop_v, send_sem=po_send, recv_sem=po_recv,
                                           device_id={'cp': partner}, device_id_type=MESH)
    po_copy.start()
    po_copy.wait()
    tcol = dmodel // chips
    for k in range(chips):
        pt_v[k] = po_v[c, :, k * tcol:(k + 1) * tcol] + pop_v[:, k * tcol:(k + 1) * tcol]

    def pt_go(r, _):
        pltpu.make_async_remote_copy(src_ref=pt_v.at[chip_at(r)], dst_ref=ptr_v.at[r - 1], send_sem=pt_send, recv_sem=pt_recv,
                                     device_id={'cp': 2 * chip_at(r) + c}, device_id_type=MESH).start()
        return 0
    lax.fori_loop(1, chips, pt_go, 0)
    pending['pt_send'] = lambda: wait_bytes(ptr_v, pt_send)
    wait_bytes(ptr_v, pt_recv)
    tot = pt_v[t]
    for r in range(chips - 1):
        tot = tot + ptr_v[r]
    ag_v[c, t] = rounded(xf_v[c, :, pl.ds(pl.multiple_of(t * tcol, LANES), tcol)] + tot)

    def ag_go(r, _):
        pltpu.make_async_remote_copy(src_ref=ag_v.at[c, t], dst_ref=ag_v.at[c, t], send_sem=ag_send, recv_sem=ag_recv,
                                     device_id={'cp': 2 * chip_at(r) + c}, device_id_type=MESH).start()
        return 0
    lax.fori_loop(1, chips, ag_go, 0)
    pending['ag_send'] = lambda: wait_bytes(ag_v.at[0, pl.ds(0, chips - 1)], ag_send)
    wait_bytes(ag_v.at[0, pl.ds(0, chips - 1)], ag_recv)
    ag_copy = pltpu.make_async_remote_copy(src_ref=ag_v.at[c], dst_ref=ag_v.at[c], send_sem=ag2_send, recv_sem=ag2_recv,
                                           device_id={'cp': partner}, device_id_type=MESH)
    ag_copy.start()
    ag_copy.wait()
    for k in range(chips):
        out_v[:, k * tcol:(k + 1) * tcol] = jnp.concatenate([ag_v[0, k], ag_v[1, k]], axis=0).astype(BF16)

    drain()


def split_outputs(packed_v, xo_v, cn_v, kr_v):
    dmodel, latent, rope = xo_v.shape[1], cn_v.shape[1], kr_v.shape[1]
    xo_v[...] = packed_v[:, :dmodel]
    cn_v[...] = packed_v[:, dmodel:dmodel + latent]
    kr_v[...] = packed_v[:, dmodel + latent:dmodel + latent + rope]


def solution(mesh):
    cp = mesh.shape['cp']
    side = math.isqrt(cp // 2)
    inner = 2 * side
    chips = cp // 2

    def decode_step(x, w_dq, g_q, w_uq, w_dkv, g_kv, w_uk, w_uv, w_o, cache_c, cache_kr, ctx_len):
        nreq, dmodel = x.shape
        qlora = w_dq.shape[1]
        latent, heads, nope = w_uk.shape
        rope = cache_kr.shape[2]
        tdev = cache_c.shape[1]
        half = heads // 2
        own = heads // cp
        wide = latent + LANES
        tcol = dmodel // chips
        inv = (np.float64(ROPE_THETA) ** (-2.0 * np.arange(rope // 2) / rope)).astype(np.float32)
        freq = np.zeros((1, LANES), np.float32)
        freq[0, :rope] = np.concatenate([inv, inv])
        anyspec = pl.BlockSpec(memory_space=pl.ANY)
        dma = pltpu.SemaphoreType.DMA
        vm = pltpu.VMEM
        out_shape = (jax.ShapeDtypeStruct((nreq, dmodel), BF16), jax.ShapeDtypeStruct((nreq, latent), BF16),
                     jax.ShapeDtypeStruct((nreq, rope), BF16))
        scratch = [
            vm((nreq, dmodel), BF16), vm((qlora,), F32),
            vm((w_uq.shape[1] // qlora, qlora, qlora // 2), BF16), vm((w_dkv.shape[1], dmodel // inner), BF16), vm((1, latent), F32),
            vm((half // 8, latent, 8, nope), BF16), vm((latent, 8, nope), BF16), vm((own * nope, dmodel), BF16),
            vm((nreq, tdev, latent), BF16), vm((nreq, rope, tdev), BF16), vm((1, LANES), F32), vm((own, latent, nope), BF16),
            vm((half, latent, nope), BF16), vm((latent * 8, nope), F32),
            vm((2, nreq // 2, dmodel), F32), vm((2, nreq, qlora // 2), F32), vm((inner, nreq, wide), F32),
            vm((wide // LANES, heads * nreq, LANES), F32), vm((nreq, wide), F32),
            vm((heads, tdev), F32), vm((heads, tdev), F32), vm((heads, LANES), F32), vm((heads, LANES), F32),
            vm((nreq, heads, wide), F32), vm((nreq, half, wide), F32),
            vm((nreq // 2, half, wide), F32), vm((nreq // 2, side - 1, half // side, wide), F32),
            vm((nreq // 2, side, own, wide), F32), vm((nreq // 2, side - 1, own, wide), F32),
            vm((nreq // 2, chips, own, wide), F32), vm((nreq // 2, chips - 1, own, wide), F32), vm((own, nreq, latent), F32),
            vm((2, nreq // 2, dmodel), F32), vm((nreq // 2, dmodel), F32),
            vm((chips, nreq // 2, tcol), F32), vm((chips - 1, nreq // 2, tcol), F32), vm((2, chips, nreq // 2, tcol), F32),
            dma((8,)), dma((dmodel // qlora,)), dma((w_uq.shape[1] // qlora,)), dma((half // 8,)), dma((2, nreq)),
            dma, dma, dma, dma, dma((half // 8,)), dma((half // 8,)), dma((nreq,)), dma((nreq,)), dma((nreq // 2,)), dma((nreq // 2,)), dma((nreq // 2,)), dma((nreq // 2,)),
            dma((nreq // 2,)), dma((nreq // 2,)),
            dma, dma, dma, dma, dma, dma, dma, dma,
        ]
        packed = pl.pallas_call(
            functools.partial(step_kernel, (cp, side)),
            out_shape=jax.ShapeDtypeStruct((nreq, dmodel + wide), BF16),
            in_specs=[anyspec] * 12 + [pl.BlockSpec(memory_space=pltpu.SMEM)],
            out_specs=pl.BlockSpec(memory_space=pltpu.VMEM),
            scratch_shapes=scratch,
            compiler_params=pltpu.CompilerParams(collective_id=0, has_side_effects=True, vmem_limit_bytes=67043328),
            name='decode_step',
        )(x, w_dq, g_q, w_uq, w_dkv.T, g_kv.reshape(1, latent), w_uk, w_uv, w_o,
          cache_c, jnp.swapaxes(cache_kr, 1, 2), jnp.asarray(freq), ctx_len)
        vspec = pl.BlockSpec(memory_space=pltpu.VMEM)
        return pl.pallas_call(split_outputs, out_shape=out_shape, in_specs=[vspec], out_specs=(vspec,) * 3,
                              name='split_outputs')(packed)

    spec_rows = P('dp', None)
    spec_cache = P('dp', 'cp', None)
    in_specs = (spec_rows, P(), P(), P(), P(), P(), P(), P(), P(), spec_cache, spec_cache, P('dp'))
    out_specs = (spec_rows, spec_rows, spec_rows)
    return jax.shard_map(decode_step, mesh=mesh, in_specs=in_specs, out_specs=out_specs, check_vma=False)
```

```python
import functools
import math

import jax
import jax.numpy as jnp
import numpy as np
from jax import lax
from jax.experimental import pallas as pl
from jax.experimental.pallas import tpu as pltpu
from jax.sharding import PartitionSpec as P

NORM_EPS = 1e-6
ROPE_THETA = 10000.0
MASKED = -1e30
FLOOR = -1e29
F32, BF16 = jnp.float32, jnp.bfloat16
MESH = pl.DeviceIdType.MESH
NT = (((1,), (1,)), ((), ()))
LANES = 128


def dot(a, b):
    return jnp.dot(a, b, preferred_element_type=F32)


def dot_nt(a, b):
    return lax.dot_general(a, b, NT, preferred_element_type=F32)


def rounded(v):
    return v.astype(BF16).astype(F32)


def wait_bytes(view, sem):
    pltpu.make_async_copy(view, view, sem).wait()


def step_kernel(dims, x_h, wdq_h, gq_h, wuq_h, wdkv_h, gkv_h, wuk_h, wuv_h, wo_h, cc_h, kr_h, freq_h, ctx_s,
                out_v,
                x_v, gq_v, wuq_v, wdkv_v, gkv_v, wuk_v, wuv_v, wo_v, cc_v, kr_v, freq_v, wv_v, wk_v, stage_v,
                xf_v, cq_v, kvp_v, q_v, cnf_v, sa_v, sb_v, ma_v, mb_v, acc_v, pair_v, xs_v, xsr_v, ys_v, ysr_v, rs_v, rsr_v, olat_v, po_v, pop_v, pt_v, ptr_v, ag_v,
                in_sem, dq_sem, uq_sem, uk_sem, cc_sem,
                a_send, a_recv, kv_send, kv_recv, q_send, q_recv, pair_send, pair_recv, xs_send, xs_recv, ys_send, ys_recv, rs_send, rs_recv,
                po_send, po_recv, pt_send, pt_recv, ag_send, ag_recv, ag2_send, ag2_recv):
    cp, side = dims
    chips = cp // 2
    inner = 2 * side
    nreq, dmodel = x_v.shape
    nslab, latent, slab, nope = wuk_v.shape
    half_heads = nslab * slab
    heads = 2 * half_heads
    rope = kr_v.shape[1]
    half_rope = rope // 2
    tdev = cc_v.shape[1]
    wide = latent + LANES
    qk = nope + rope
    kdkv = wdkv_v.shape[1]
    own = heads // cp

    d = lax.axis_index('cp')
    c = lax.rem(d, 2)
    t = d // 2
    oc = 1 - c
    gi = lax.rem(d, inner)
    base = d - gi
    xx = gi // 2
    yy = d // inner
    partner = base + 2 * xx + oc

    kstep = 64

    def widen(src):
        def go(i, _):
            r = pl.multiple_of(i * kstep, kstep)
            stage_v[pl.ds(pl.multiple_of(r * slab, kstep * slab), kstep * slab), :] = (
                src[pl.ds(r, kstep)].astype(F32).reshape(kstep * slab, nope))
            return 0
        lax.fori_loop(0, latent // kstep, go, 0)

    def chip_at(r):
        return lax.rem(t + r, chips)

    pending = {}

    def done(name):
        pending.pop(name)()

    def drain():
        for name in list(pending):
            done(name)

    def local(name, src, dst, sem):
        cpy = pltpu.make_async_copy(src, dst, sem)
        cpy.start()
        pending[name] = cpy.wait

    local('x', x_h, x_v, in_sem.at[0])
    nslot, krow, ucol = wuq_v.shape
    ndq = dmodel // krow
    local('gq', gq_h, gq_v, in_sem.at[3])
    local('gkv', gkv_h, gkv_v, in_sem.at[4])
    local('freq', freq_h, freq_v, in_sem.at[5])
    nuq = wuq_h.shape[1] // 2 // ucol

    def uq_copy(j):
        return pltpu.make_async_copy(wuq_h.at[:, pl.ds(pl.multiple_of((c * nuq + j) * ucol, LANES), ucol)],
                                     wuq_v.at[lax.rem(ndq + j, nslot)], uq_sem.at[j])

    def uk_copy(s):
        return pltpu.make_async_copy(wuk_h.at[:, pl.ds(pl.multiple_of(c * half_heads + s * slab, slab), slab), :],
                                     wuk_v.at[s], uk_sem.at[s])

    def cache_copies(b):
        return (pltpu.make_async_copy(cc_h.at[b], cc_v.at[b], cc_sem.at[0, b]),
                pltpu.make_async_copy(kr_h.at[b], kr_v.at[b], cc_sem.at[1, b]))

    def cache_start(b):
        for cpy in cache_copies(b):
            cpy.start()

    def cache_wait(b):
        for cpy in cache_copies(b):
            cpy.wait()

    head0 = c * half_heads + xx * slab + yy * own
    head_slab = head0 // slab
    head_in = head0 - head_slab * slab

    for s in range(nslab):
        uk_copy(s).start()
    for j in range(ndq):
        pltpu.make_async_copy(wdq_h.at[pl.ds(j * krow, krow), pl.ds(pl.multiple_of(c * ucol, LANES), ucol)],
                              wuq_v.at[j], dq_sem.at[j]).start()
    local('dkv', wdkv_h.at[:, pl.ds(pl.multiple_of(gi * kdkv, LANES), kdkv)], wdkv_v, in_sem.at[2])

    barrier = pltpu.get_barrier_semaphore()

    def greet(r, _):
        pl.semaphore_signal(barrier, inc=1, device_id={'cp': 2 * chip_at(r) + c}, device_id_type=MESH)
        return 0

    lax.fori_loop(1, chips, greet, 0)
    for i in range(side):
        pl.semaphore_signal(barrier, inc=1, device_id={'cp': base + 2 * i + oc}, device_id_type=MESH)

    def uk_step(s, _):
        uk_copy(s).wait()
        widen(wuk_v.at[s])

        def head_step(i, _):
            wk_v[s * slab + i] = stage_v[pl.ds(i, latent, stride=slab), :].astype(BF16)
            return 0
        lax.fori_loop(0, slab, head_step, 0)
        return 0

    lax.fori_loop(0, nslab, uk_step, 0)
    for j in range(2):
        uq_copy(j).start()

    done('x')
    def a_step(j, part):
        pltpu.make_async_copy(wuq_v.at[j], wuq_v.at[j], dq_sem.at[j]).wait()

        @pl.when(j < nslot - ndq - 2)
        def _():
            uq_copy(j + 2).start()
        return part + dot(x_v[:, pl.ds(pl.multiple_of(j * krow, krow), krow)], wuq_v[j])

    part = lax.fori_loop(0, ndq, a_step, jnp.zeros((nreq, ucol), F32))
    cq_v[c] = part
    pl.semaphore_wait(barrier, chips - 1 + side)
    cq_copy = pltpu.make_async_remote_copy(src_ref=cq_v.at[c], dst_ref=cq_v.at[c], send_sem=a_send, recv_sem=a_recv,
                                           device_id={'cp': partner}, device_id_type=MESH)
    cq_copy.start()
    for j in range(nslot - ndq, nuq):
        uq_copy(j).start()
    pending['cq'] = cq_copy.wait

    def to_ring(buf, send, recv):
        def go(r, _):
            peer = lax.rem(gi + r, inner)
            pltpu.make_async_remote_copy(src_ref=buf.at[gi], dst_ref=buf.at[gi], send_sem=send, recv_sem=recv,
                                         device_id={'cp': base + peer}, device_id_type=MESH).start()
            return 0
        lax.fori_loop(1, inner, go, 0)

    done('dkv')
    kvp_v[gi, :, 0:latent + rope] = dot_nt(x_v[:, pl.ds(pl.multiple_of(gi * kdkv, LANES), kdkv)], wdkv_v[...])
    kvp_v[gi, :, latent + rope:] = jnp.zeros((nreq, wide - latent - rope), F32)
    to_ring(kvp_v, kv_send, kv_recv)
    pending['kv_send'] = lambda: wait_bytes(kvp_v.at[pl.ds(0, inner - 1)], kv_send)
    pending['kv_recv'] = lambda: wait_bytes(kvp_v.at[pl.ds(0, inner - 1)], kv_recv)

    xall = x_v[...].astype(F32)
    for i in range(2):
        xf_v[i] = xall[4 * i:4 * i + 4, :]
    rows = lax.broadcasted_iota(jnp.int32, (nreq, LANES), 0)
    ctx = jnp.zeros((nreq, LANES), jnp.int32)
    for b in range(nreq):
        ctx = jnp.where(rows == b, ctx_s[b], ctx)
    done('freq')
    angles = ctx.astype(F32) * freq_v[...]
    cos_full = jnp.cos(angles)[:, :rope]
    sin_raw = jnp.sin(angles)[:, :rope]
    lane = lax.broadcasted_iota(jnp.int32, (nreq, rope), 1)
    sin_full = jnp.where(lane < half_rope, -sin_raw, sin_raw)

    def rope_rotate(v):
        swapped = jnp.concatenate([v[:, half_rope:], v[:, :half_rope]], axis=1)
        return v * cos_full + swapped * sin_full

    done('cq')
    cq = rounded(jnp.concatenate([cq_v[0], cq_v[1]], axis=1))
    done('gq')
    mean_sq = jnp.mean(cq * cq, axis=1, keepdims=True)
    cn = (cq * lax.rsqrt(mean_sq + NORM_EPS) * gq_v[...].reshape(1, gq_v.shape[0])).astype(BF16)
    row0 = c * half_heads * nreq
    zeros_pad = jnp.zeros((nreq, LANES - rope), F32)
    per = ucol // qk

    def q_slab_copy(s):
        view = q_v.at[:, pl.ds(pl.multiple_of(row0 + s * slab * nreq, slab * nreq), slab * nreq)]
        return pltpu.make_async_remote_copy(src_ref=view, dst_ref=view, send_sem=q_send.at[s], recv_sem=q_recv.at[s],
                                            device_id={'cp': partner}, device_id_type=MESH)

    def q_latent(j, qc):
        for i in range(per):
            h = j * per + i
            r = pl.multiple_of(row0 + h * nreq, nreq)
            qr = rounded(rope_rotate(qc[:, i * qk + nope:(i + 1) * qk]))
            q_v[latent // LANES, pl.ds(r, nreq), :] = jnp.concatenate([qr, zeros_pad], axis=1)
            ql = rounded(dot_nt(qc[:, i * qk:i * qk + nope].astype(BF16), wk_v[h]))
            for k in range(latent // LANES):
                q_v[k, pl.ds(r, nreq), :] = ql[:, k * LANES:(k + 1) * LANES]
    def b_step(j, last):
        uq_copy(j).wait()
        cache_start(j - 1)
        qc = rounded(dot(cn, wuq_v[lax.rem(ndq + j, nslot)]))
        q_latent(j - 1, last)

        @pl.when(lax.rem(j * per, slab) == 0)
        def _():
            q_slab_copy(j * per // slab - 1).start()
        return qc

    uq_copy(0).wait()
    qc = lax.fori_loop(1, nuq, b_step, rounded(dot(cn, wuq_v[ndq])))
    cache_start(nuq - 1)
    q_latent(nuq - 1, qc)
    q_slab_copy(nslab - 1).start()
    for s in range(nslab):
        pending['q', s] = q_slab_copy(s).wait
    local('uv', wuv_h.at[:, pl.ds(pl.multiple_of(head_slab * slab, slab), slab), :], wuv_v, in_sem.at[6])
    local('wo', wo_h.at[pl.ds(pl.multiple_of(head0 * nope, own * nope), own * nope), :], wo_v, in_sem.at[7])

    done('kv_recv')
    kv = kvp_v[0]
    for i in range(1, inner):
        kv = kv + kvp_v[i]
    kvl = kv[:, :latent]
    done('gkv')
    mean_sq = jnp.mean(kvl * kvl, axis=1, keepdims=True)
    c_new = kvl * lax.rsqrt(mean_sq + NORM_EPS) * gkv_v[...]
    kr_new = rope_rotate(kv[:, latent:latent + rope])
    out_v[:, dmodel:dmodel + latent] = c_new.astype(BF16)
    out_v[:, dmodel + latent:] = jnp.concatenate([kr_new, zeros_pad], axis=1).astype(BF16)
    cnf_v[:, :latent] = rounded(c_new)
    cnf_v[:, latent:] = jnp.concatenate([rounded(kr_new), zeros_pad], axis=1)

    for s in range(nslab):
        done(('q', s))

    scale = (nope + rope) ** -0.5
    block0 = d * tdev
    head_row = lax.broadcasted_iota(jnp.int32, (heads, 1), 0)
    mine0 = pl.multiple_of(c * half_heads, half_heads)
    theirs0 = pl.multiple_of(oc * half_heads, half_heads)

    def pair_copy(b):
        return pltpu.make_async_remote_copy(src_ref=acc_v.at[b, pl.ds(theirs0, half_heads)], dst_ref=pair_v.at[b],
                                            send_sem=pair_send.at[b], recv_sem=pair_recv.at[b],
                                            device_id={'cp': partner}, device_id_type=MESH)

    nkc = 4
    kc = tdev // nkc
    half_lane = lax.broadcasted_iota(jnp.int32, (heads, LANES), 1) < LANES // 2
    chunk_pos = lax.broadcasted_iota(jnp.int32, (heads, kc), 1)

    def q_of(b):
        return jnp.concatenate([q_v[k, pl.ds(b, heads, stride=nreq), :] for k in range(wide // LANES)], axis=1)

    def scores(b, s_ref, m_ref):
        qb = q_of(b).astype(BF16)
        left = ctx_s[b] - block0
        m = None
        for k in range(nkc):
            cols = slice(k * kc, (k + 1) * kc)
            s = (dot_nt(qb[:, :latent], cc_v[b, cols]) + dot(qb[:, latent:latent + rope], kr_v[b, :, cols])) * scale
            s = jnp.where(chunk_pos < left - k * kc, s, MASKED)
            s_ref[:, cols] = s
            mk = jnp.max(s, axis=1, keepdims=True)
            m = mk if m is None else jnp.maximum(m, mk)
        m_ref[...] = jnp.broadcast_to(m, (heads, LANES))

    def weigh(b, s_ref, m_ref):
        qf = q_of(b)
        left = ctx_s[b] - block0
        new_row = cnf_v[pl.ds(b, 1), :]
        new_s = jnp.sum(qf * new_row, axis=1, keepdims=True) * scale
        at = head_row * 0 + left
        new_s = jnp.where(jnp.logical_and(at >= 0, at < tdev), new_s, MASKED)
        m = jnp.maximum(jnp.maximum(m_ref[:, :1], new_s), FLOOR)
        new_w = jnp.exp(new_s - m)
        l = new_w
        acc = rounded(new_w) * new_row[:, :latent]
        for k in range(nkc):
            cols = slice(k * kc, (k + 1) * kc)
            p = jnp.exp(s_ref[:, cols] - m)
            l = l + jnp.sum(p, axis=1, keepdims=True)
            acc = acc + dot(p.astype(BF16), cc_v[b, cols])
        acc_v[b, :, :latent] = acc
        acc_v[b, :, latent:] = jnp.where(half_lane, m, l)

    quarter = half_heads // side

    def ring_peer(axis, r):
        if axis == 0:
            p = lax.rem(xx + r, side)
            return p, base + 2 * p + c
        p = lax.rem(yy + r, side)
        return p, p * inner + gi

    here = (xx, yy)

    def xs_copy(b, axis, r):
        p, dev = ring_peer(axis, r)
        return pltpu.make_async_remote_copy(src_ref=xs_v.at[b, pl.ds(pl.multiple_of(p * quarter, quarter), quarter)],
                                            dst_ref=xsr_v.at[b, r - 1], send_sem=xs_send.at[b], recv_sem=xs_recv.at[b],
                                            device_id={'cp': dev}, device_id_type=MESH)

    def ys_copy(b, axis, r):
        p, dev = ring_peer(1 - axis, r)
        return pltpu.make_async_remote_copy(src_ref=ys_v.at[b, p], dst_ref=ysr_v.at[b, r - 1],
                                            send_sem=ys_send.at[b], recv_sem=ys_recv.at[b],
                                            device_id={'cp': dev}, device_id_type=MESH)

    def ml_of(v):
        return v[:, latent:latent + 1], v[:, wide - 1:wide]

    def merge(parts):
        ms, ls = zip(*[ml_of(p) for p in parts])
        m = functools.reduce(jnp.maximum, ms)
        fs = [jnp.exp(mi - m) for mi in ms]
        l = sum(f * li for f, li in zip(fs, ls))
        acc = sum(f * p[:, :latent] for f, p in zip(fs, parts))
        return m, l, acc

    def with_ml(m, l):
        side_lane = lax.broadcasted_iota(jnp.int32, (m.shape[0], LANES), 1)
        return jnp.where(side_lane < LANES // 2, m, l)

    nring = nreq // 2

    def rs_copy(b, r):
        p = chip_at(r)
        return pltpu.make_async_remote_copy(src_ref=rs_v.at[b - nring, lax.rem(p, side) * side + p // side],
                                            dst_ref=rsr_v.at[b - nring, r - 1],
                                            send_sem=rs_send.at[b - nring], recv_sem=rs_recv.at[b - nring],
                                            device_id={'cp': 2 * p + c}, device_id_type=MESH)

    def direct_step(b):
        pair_copy(b).wait_recv()
        m, l, acc = merge([acc_v[b, pl.ds(mine0, half_heads), :], pair_v[b]])
        ml = with_ml(m, l)
        for k in range(chips):
            rs_v[b - nring, k, :, :latent] = acc[own * k:own * (k + 1), :]
            rs_v[b - nring, k, :, latent:] = ml[own * k:own * (k + 1), :]

        def go(r, _):
            rs_copy(b, r).start()
            return 0
        lax.fori_loop(1, chips, go, 0)

    def pair_step(b, axis):
        pair_copy(b).wait_recv()
        m, l, acc = merge([acc_v[b, pl.ds(mine0, half_heads), :], pair_v[b]])
        ml = with_ml(m, l)
        if axis == 0:
            xs_v[b, :, :latent] = acc
            xs_v[b, :, latent:] = ml
        else:
            for p in range(side):
                for k in range(side):
                    src = slice(p * quarter + k * own, p * quarter + (k + 1) * own)
                    dst = slice(k * quarter + p * own, k * quarter + (p + 1) * own)
                    xs_v[b, dst, :latent] = acc[src]
                    xs_v[b, dst, latent:] = ml[src]
        for r in range(1, side):
            xs_copy(b, axis, r).start()

    def ring_merge(b, axis):
        mine = xs_v[b, pl.ds(pl.multiple_of(here[axis] * quarter, quarter), quarter), :]
        m, l, acc = merge([mine] + [xsr_v[b, r] for r in range(side - 1)])
        ml = with_ml(m, l)
        for k in range(side):
            ys_v[b, k, :, :latent] = acc[own * k:own * (k + 1), :]
            ys_v[b, k, :, latent:] = ml[own * k:own * (k + 1), :]

    def ring_step(i):
        for k in range(2):
            wait_bytes(xsr_v.at[2 * i + k], xs_recv.at[2 * i + k])
        for k in range(2):
            ring_merge(2 * i + k, k)
        for k in range(2):
            for r in range(1, side):
                ys_copy(2 * i + k, k, r).start()

    def two_requests(i, _):
        b = 2 * i
        cache_wait(b + 1)
        scores(b + 1, sb_v, mb_v)
        weigh(b, sa_v, ma_v)
        pair_copy(b).start()

        @pl.when(jnp.logical_and(b - 1 > 0, b - 1 < nring))
        def _():
            pair_step(b - 1, 1)

        @pl.when(b - 1 >= nring)
        def _():
            direct_step(b - 1)

        @pl.when(b + 2 < nreq)
        def _():
            cache_wait(b + 2)
        scores(jnp.minimum(b + 2, nreq - 1), sa_v, ma_v)
        weigh(b + 1, sb_v, mb_v)
        pair_copy(b + 1).start()
        @pl.when(b < nring)
        def _():
            pair_step(b, 0)

        @pl.when(b >= nring)
        def _():
            direct_step(b)
            ring_step(i - nring // 2)
        return 0

    cache_wait(0)
    scores(0, sa_v, ma_v)
    lax.fori_loop(0, nreq // 2, two_requests, 0)
    for b in range(nreq):
        pending['pair', b] = pair_copy(b).wait_send

    direct_step(nreq - 1)

    def each(view, sem):
        def go(b, _):
            wait_bytes(view.at[b], sem.at[b])
            return 0
        return lambda: lax.fori_loop(0, nring, go, 0)

    pending['xs_send'] = each(xsr_v, xs_send)
    pending['ys_send'] = each(ysr_v, ys_send)
    pending['ys_recv'] = each(ysr_v, ys_recv)
    pending['rs_send'] = each(rsr_v, rs_send)
    pending['rs_recv'] = each(rsr_v, rs_recv)

    done('uv')
    widen(wuv_v)
    for k in range(own):
        wv_v[k] = stage_v[pl.ds(head_in + k, latent, stride=slab), :].astype(BF16)

    def put(b, acc, l):
        ol = rounded(acc / l)
        for k in range(own):
            olat_v[k, b:b + 1, :] = ol[k:k + 1, :]

    done('ys_recv')
    for b in range(nring):
        m, l, acc = merge([ys_v[b, here[1 - b % 2]]] + [ysr_v[b, r] for r in range(side - 1)])
        put(b, acc, l)
    pending.pop('rs_recv')
    for b in range(nring):
        wait_bytes(rsr_v.at[b], rs_recv.at[b])
        m, l, acc = merge([rs_v[b, xx * side + yy]] + [rsr_v[b, r] for r in range(chips - 1)])
        put(nring + b, acc, l)

    done('wo')
    outs = []
    for k in range(own):
        outs.append(dot(olat_v[k].astype(BF16), wv_v[k]).astype(BF16))
    o = jnp.concatenate(outs, axis=1)
    ncol = dmodel // 8

    def po_copy(k):
        cols = pl.ds(k * (dmodel // 2), dmodel // 2)
        return pltpu.make_async_remote_copy(src_ref=po_v.at[oc, :, cols], dst_ref=pop_v.at[:, cols], send_sem=po_send.at[k],
                                            recv_sem=po_recv.at[k], device_id={'cp': partner}, device_id_type=MESH)

    for j in range(8):
        pj = dot(o, wo_v[:, j * ncol:(j + 1) * ncol])
        for i in range(2):
            po_v[i, :, j * ncol:(j + 1) * ncol] = pj[4 * i:4 * i + 4, :]
        if j % 4 == 3:
            po_copy(j // 4).start()
    for k in range(2):
        po_copy(k).wait()
    tcol = dmodel // chips
    for k in range(chips):
        pt_v[k] = po_v[c, :, k * tcol:(k + 1) * tcol] + pop_v[:, k * tcol:(k + 1) * tcol]

    def pt_go(r, _):
        pltpu.make_async_remote_copy(src_ref=pt_v.at[chip_at(r)], dst_ref=ptr_v.at[r - 1], send_sem=pt_send, recv_sem=pt_recv,
                                     device_id={'cp': 2 * chip_at(r) + c}, device_id_type=MESH).start()
        return 0
    lax.fori_loop(1, chips, pt_go, 0)
    pending['pt_send'] = lambda: wait_bytes(ptr_v, pt_send)
    wait_bytes(ptr_v, pt_recv)
    tot = pt_v[t]
    for r in range(chips - 1):
        tot = tot + ptr_v[r]
    ag_v[c, t] = rounded(xf_v[c, :, pl.ds(pl.multiple_of(t * tcol, LANES), tcol)] + tot)

    def ag_go(r, _):
        pltpu.make_async_remote_copy(src_ref=ag_v.at[c, t], dst_ref=ag_v.at[c, t], send_sem=ag_send, recv_sem=ag_recv,
                                     device_id={'cp': 2 * chip_at(r) + c}, device_id_type=MESH).start()
        return 0
    lax.fori_loop(1, chips, ag_go, 0)
    pending['ag_send'] = lambda: wait_bytes(ag_v.at[0, pl.ds(0, chips - 1)], ag_send)
    wait_bytes(ag_v.at[0, pl.ds(0, chips - 1)], ag_recv)
    ag_copy = pltpu.make_async_remote_copy(src_ref=ag_v.at[c], dst_ref=ag_v.at[c], send_sem=ag2_send, recv_sem=ag2_recv,
                                           device_id={'cp': partner}, device_id_type=MESH)
    ag_copy.start()
    ag_copy.wait()
    for k in range(chips):
        out_v[:, k * tcol:(k + 1) * tcol] = jnp.concatenate([ag_v[0, k], ag_v[1, k]], axis=0).astype(BF16)

    drain()


def split_outputs(packed_v, xo_v, cn_v, kr_v):
    dmodel, latent, rope = xo_v.shape[1], cn_v.shape[1], kr_v.shape[1]
    xo_v[...] = packed_v[:, :dmodel]
    cn_v[...] = packed_v[:, dmodel:dmodel + latent]
    kr_v[...] = packed_v[:, dmodel + latent:dmodel + latent + rope]


def solution(mesh):
    cp = mesh.shape['cp']
    side = math.isqrt(cp // 2)
    inner = 2 * side
    chips = cp // 2

    def decode_step(x, w_dq, g_q, w_uq, w_dkv, g_kv, w_uk, w_uv, w_o, cache_c, cache_kr, ctx_len):
        nreq, dmodel = x.shape
        qlora = w_dq.shape[1]
        latent, heads, nope = w_uk.shape
        rope = cache_kr.shape[2]
        tdev = cache_c.shape[1]
        half = heads // 2
        own = heads // cp
        wide = latent + LANES
        tcol = dmodel // chips
        inv = (np.float64(ROPE_THETA) ** (-2.0 * np.arange(rope // 2) / rope)).astype(np.float32)
        freq = np.zeros((1, LANES), np.float32)
        freq[0, :rope] = np.concatenate([inv, inv])
        anyspec = pl.BlockSpec(memory_space=pl.ANY)
        dma = pltpu.SemaphoreType.DMA
        vm = pltpu.VMEM
        out_shape = (jax.ShapeDtypeStruct((nreq, dmodel), BF16), jax.ShapeDtypeStruct((nreq, latent), BF16),
                     jax.ShapeDtypeStruct((nreq, rope), BF16))
        scratch = [
            vm((nreq, dmodel), BF16), vm((qlora,), F32),
            vm((w_uq.shape[1] // qlora, qlora, qlora // 2), BF16), vm((w_dkv.shape[1], dmodel // inner), BF16), vm((1, latent), F32),
            vm((half // 8, latent, 8, nope), BF16), vm((latent, 8, nope), BF16), vm((own * nope, dmodel), BF16),
            vm((nreq, tdev, latent), BF16), vm((nreq, rope, tdev), BF16), vm((1, LANES), F32), vm((own, latent, nope), BF16),
            vm((half, latent, nope), BF16), vm((latent * 8, nope), F32),
            vm((2, nreq // 2, dmodel), F32), vm((2, nreq, qlora // 2), F32), vm((inner, nreq, wide), F32),
            vm((wide // LANES, heads * nreq, LANES), F32), vm((nreq, wide), F32),
            vm((heads, tdev), F32), vm((heads, tdev), F32), vm((heads, LANES), F32), vm((heads, LANES), F32),
            vm((nreq, heads, wide), F32), vm((nreq, half, wide), F32),
            vm((nreq // 2, half, wide), F32), vm((nreq // 2, side - 1, half // side, wide), F32),
            vm((nreq // 2, side, own, wide), F32), vm((nreq // 2, side - 1, own, wide), F32),
            vm((nreq // 2, chips, own, wide), F32), vm((nreq // 2, chips - 1, own, wide), F32), vm((own, nreq, latent), F32),
            vm((2, nreq // 2, dmodel), F32), vm((nreq // 2, dmodel), F32),
            vm((chips, nreq // 2, tcol), F32), vm((chips - 1, nreq // 2, tcol), F32), vm((2, chips, nreq // 2, tcol), F32),
            dma((8,)), dma((dmodel // qlora,)), dma((w_uq.shape[1] // qlora,)), dma((half // 8,)), dma((2, nreq)),
            dma, dma, dma, dma, dma((half // 8,)), dma((half // 8,)), dma((nreq,)), dma((nreq,)), dma((nreq // 2,)), dma((nreq // 2,)), dma((nreq // 2,)), dma((nreq // 2,)),
            dma((nreq // 2,)), dma((nreq // 2,)),
            dma((2,)), dma((2,)), dma, dma, dma, dma, dma, dma,
        ]
        packed = pl.pallas_call(
            functools.partial(step_kernel, (cp, side)),
            out_shape=jax.ShapeDtypeStruct((nreq, dmodel + wide), BF16),
            in_specs=[anyspec] * 12 + [pl.BlockSpec(memory_space=pltpu.SMEM)],
            out_specs=pl.BlockSpec(memory_space=pltpu.VMEM),
            scratch_shapes=scratch,
            compiler_params=pltpu.CompilerParams(collective_id=0, has_side_effects=True, vmem_limit_bytes=67043328),
            name='decode_step',
        )(x, w_dq, g_q, w_uq, w_dkv.T, g_kv.reshape(1, latent), w_uk, w_uv, w_o,
          cache_c, jnp.swapaxes(cache_kr, 1, 2), jnp.asarray(freq), ctx_len)
        vspec = pl.BlockSpec(memory_space=pltpu.VMEM)
        return pl.pallas_call(split_outputs, out_shape=out_shape, in_specs=[vspec], out_specs=(vspec,) * 3,
                              name='split_outputs')(packed)

    spec_rows = P('dp', None)
    spec_cache = P('dp', 'cp', None)
    in_specs = (spec_rows, P(), P(), P(), P(), P(), P(), P(), P(), spec_cache, spec_cache, P('dp'))
    out_specs = (spec_rows, spec_rows, spec_rows)
    return jax.shard_map(decode_step, mesh=mesh, in_specs=in_specs, out_specs=out_specs, check_vma=False)
```
